128 devices in a mesh: vocab: 64 (over x, y, z), width: 2 (over core).
Axes of the slice: x: 4, y: 4, z: 4, core: 2. Of those that a mesh axis runs over, the one named last changes fastest.
Arguments:
- token_grads: bfloat16 [65536, 4608], P('vocab', 'width'), may hold values from -6 to 6
- token_slot: int32 [65536], P('vocab'), may hold values from 0 to 1023, as said below
- slot_rows: int32 [64, 1024], P('vocab'), may hold values from 0 to 1023, as said below
- counts: int32 [64, 64], P('vocab'), may hold values from 1 to 16, as said below
- weights: bfloat16 [65536, 4608], P('vocab', 'width'), may hold values from -0.29882812 to 0.29882812
- moment: bfloat16 [65536, 4608], P('vocab', 'width'), may hold values from -2 to 2
- row_scale: float32 [65536], P('vocab'), may hold values from 0.1 to 4
- row_steps: int32 [65536], P('vocab'), may hold values from 0 to 11
Outputs:
- new_weights: bfloat16 [65536, 4608], P('vocab', 'width')
- new_moment: bfloat16 [65536, 4608], P('vocab', 'width')
- new_scale: float32 [65536], P('vocab')
The draws below stay inside these ranges and needn't reach their ends.
Inputs may be any that keep to these rules, and one draw needn't show every extreme that they name: `token_slot`: each token names a live slot of its own source. `slot_rows`: within one source and one owner the 16 entries are distinct. `counts`: in every draw some owners receive 16 live slots from every source.
All inputs are finite; a program needn't handle non-finite values.
Results may differ from the reference program's by a relative error of at most 0.0011.
Values may be sent and summed in bfloat16 or wider, within the bound.
A program may use at most 128 MiB of HBM per device.

```python
import math
import jax
import jax.numpy as jnp
from jax import lax

D = 4608
VOC_DEV = 1024
CAP = 16
TOK_DEV = 1024
OWNERS = 64
TOKENS = 65536
VOCAB = 65536


def routing(key):
    base = jax.random.fold_in(key, 7)
    key_hot, key_small, key_rows, key_pick = jax.random.split(base, 4)
    hot = jax.random.permutation(key_hot, OWNERS) < max(OWNERS // 8, 1)
    small = jax.random.randint(key_small, (OWNERS, OWNERS), 1, max(CAP // 4, 1) + 1)
    counts = jnp.where(hot[None, :], CAP, small).astype(jnp.int32)
    row_keys = jax.random.split(key_rows, OWNERS * OWNERS)
    picked = jax.vmap(lambda k: jax.random.permutation(k, VOC_DEV)[:CAP])(row_keys)
    slot_rows = picked.reshape(OWNERS, OWNERS * CAP).astype(jnp.int32)
    within = jnp.arange(CAP, dtype=jnp.int32)
    live = (within[None, None, :] < counts[:, :, None]).reshape(OWNERS, OWNERS * CAP)
    order_key = jnp.where(live, 0, 1) * (OWNERS * CAP) + jnp.arange(OWNERS * CAP, dtype=jnp.int32)[None, :]
    order = jnp.argsort(order_key, axis=1, stable=True).astype(jnp.int32)
    live_count = jnp.sum(live.astype(jnp.int32), axis=1)
    raw = jax.random.randint(key_pick, (OWNERS, TOK_DEV), 0, 1 << 30)
    pick = raw % live_count[:, None]
    token_slot = jnp.take_along_axis(order, pick, axis=1).reshape(TOKENS).astype(jnp.int32)
    return (token_slot, slot_rows, counts)


def draw_token_slot(key, part):
    return routing(key)[0]


def draw_slot_rows(key, part):
    return routing(key)[1]


def draw_counts(key, part):
    return routing(key)[2]


def set_ends(values, key, smallest, largest):
    dims = values.shape
    place = [jax.random.randint(jax.random.fold_in(key, axis), (), 0, dims[axis]) for axis in range(len(dims))]
    values = values.at[tuple(place)].set(smallest)
    longest = dims.index(max(dims))
    place[longest] = (place[longest] + 1) % dims[longest]
    return values.at[tuple(place)].set(largest)


def levels(stream_key, shape, cuts, least, largest):
    factor_of, own = 1.0, jax.random.fold_in(stream_key, 6)
    for axis_at, parts in cuts:
        draws = jnp.exp(jax.random.uniform(jax.random.fold_in(own, axis_at), (parts,), jnp.float32, least / len(cuts), largest / len(cuts)))
        factor_of = factor_of * jnp.repeat(draws, shape[axis_at] // parts).reshape([-1 if axis == axis_at else 1 for axis in range(len(shape))])
    return factor_of


def scatter_about(own_key, shape, deviation, limit, cuts=(), kind=jnp.bfloat16):
    level = levels(own_key, shape, cuts, -0.22, 0.18) if cuts else 1.0
    entries = jax.random.normal(own_key, shape, jnp.float32) * deviation * level
    return jnp.minimum(jnp.maximum(entries, -limit), limit).astype(kind)


def setup_inputs(seed: int = 0) -> dict:
    streams_of = jax.random.split(jax.random.key(seed), 9)
    token_grads = scatter_about(streams_of[0], (TOKENS, D), 1.0, 6.0, ((0, 64), (1, 2)))
    token_slot = draw_token_slot(jax.random.fold_in(streams_of[8], 71), 0)
    slot_rows = draw_slot_rows(jax.random.fold_in(streams_of[8], 71), 0)
    counts = draw_counts(jax.random.fold_in(streams_of[8], 71), 0)
    weights = scatter_about(streams_of[4], (VOCAB, D), 0.05, 0.29882812, ((0, 64), (1, 2)))
    moment = scatter_about(streams_of[5], (VOCAB, D), 0.3, 2.0, ((0, 64), (1, 2)))
    row_scale = jnp.clip(jnp.exp(math.log(4.0) - 3.6888794 * jax.random.uniform(streams_of[6], (VOCAB,), jnp.float32) ** levels(streams_of[6], (VOCAB,), ((0, 64),), -0.2, 0.2)), 0.1, 4.0)
    row_steps = set_ends(jax.random.randint(streams_of[7], (VOCAB,), 0, 12), jax.random.fold_in(streams_of[7], 1), 0, 11).astype(jnp.int32)
    return {"token_grads": token_grads, "token_slot": token_slot, "slot_rows": slot_rows, "counts": counts, "weights": weights, "moment": moment, "row_scale": row_scale, "row_steps": row_steps}


def reference(token_grads, token_slot, slot_rows, counts, weights, moment, row_scale, row_steps):
    slots_all = OWNERS * CAP
    source = jnp.arange(TOKENS, dtype=jnp.int32) // TOK_DEV
    segment = source * slots_all + token_slot
    slot_grads = jax.ops.segment_sum(token_grads.astype(jnp.float32), segment, num_segments=OWNERS * slots_all).astype(jnp.bfloat16)
    position = jnp.arange(slots_all, dtype=jnp.int32)
    owner = position // CAP
    within = position % CAP
    live = within[None, :] < jnp.take_along_axis(counts, jnp.broadcast_to(owner[None, :], (OWNERS, slots_all)), axis=1)
    target = jnp.where(live, owner[None, :] * VOC_DEV + slot_rows, VOCAB).reshape(-1)
    grad = jax.ops.segment_sum(slot_grads.astype(jnp.float32), target, num_segments=VOCAB + 1)[:VOCAB]
    hits = jax.ops.segment_sum(jnp.ones_like(target), target, num_segments=VOCAB + 1)[:VOCAB]
    touched = hits > 0
    square = lax.optimization_barrier(jnp.sum(grad * grad, axis=1)) / D
    step_count = (row_steps + 1).astype(jnp.float32)
    first = 0.9 * moment.astype(jnp.float32) + 0.1 * grad
    second = 0.95 * row_scale + 0.05 * square
    first = jnp.where(touched[:, None], first, moment.astype(jnp.float32))
    second = jnp.where(touched, second, row_scale)
    fix_first = 1.0 - jnp.power(jnp.float32(0.9), step_count)
    fix_second = 1.0 - jnp.power(jnp.float32(0.95), step_count)
    denom = jnp.sqrt(second / fix_second) + 1e-08
    old = weights.astype(jnp.float32)
    stepped = old - 0.01 * (first / fix_first[:, None] / denom[:, None] + 0.1 * old)
    new_weights = jnp.where(touched[:, None], stepped, old).astype(jnp.bfloat16)
    return (new_weights, first.astype(jnp.bfloat16), second)
```

```python
import functools
import jax
import jax.numpy as jnp
from jax import lax
from jax.experimental import pallas as pl
from jax.experimental.pallas import tpu as pltpu
from jax.sharding import PartitionSpec as P

D = 4608
HALF = 2304
ROWS = 1024
CAP = 16
GROUPS = 3
PER = 3
CW = HALF // (GROUPS * PER)
CHUNKS = GROUPS * PER
MESH = pl.DeviceIdType.MESH
ORDERS = ((0, 1, 2), (1, 2, 0), (2, 0, 1))


def to_column(row):
    eye = lax.broadcasted_iota(jnp.int32, (128, 128), 0) == lax.broadcasted_iota(jnp.int32, (128, 128), 1)
    parts = [
        jnp.sum(jnp.where(eye, row[g : g + 1, :], 0.0), axis=1, keepdims=True) for g in range(8)
    ]
    return jnp.concatenate(parts, axis=0)


def to_row(column):
    eye = lax.broadcasted_iota(jnp.int32, (128, 128), 0) == lax.broadcasted_iota(jnp.int32, (128, 128), 1)
    parts = [
        jnp.sum(jnp.where(eye, column[g * 128 : g * 128 + 128, :], 0.0), axis=0, keepdims=True)
        for g in range(8)
    ]
    return jnp.concatenate(parts, axis=0)


def exchange(
    tg, ts, srows, cnts, rscale, rsteps,
    grad, coef, scale,
    tgv, send, r1, r2, r3, onehot, ms, m1, m2, m3, acc, sq_out, sq_in,
    load_sem, send_sem, recv_sem, msend_sem, mrecv_sem, sq_sem,
):
    me = lax.axis_index("vocab")
    core = lax.axis_index("width")
    at = (me // 16, (me // 4) % 4, me % 4)
    stride = (16, 4, 1)

    def peer(dim, delta):
        there = (at[dim] + delta) % 4
        return there, (me + (there - at[dim]) * stride[dim], core)

    def load(c):
        return pltpu.make_async_copy(tg.at[:, pl.ds(c * CW, CW)], tgv.at[c], load_sem.at[c])

    issue = [g * PER + k for k in range(PER) for g in range(GROUPS)]
    for c in issue:
        load(c).start()

    barrier = pltpu.get_barrier_semaphore()
    for dim in range(3):
        for delta in (1, 2, 3):
            pl.semaphore_signal(barrier, inc=1, device_id=peer(dim, delta)[1], device_id_type=MESH)
    partner = (me, 1 - core)
    pl.semaphore_signal(barrier, inc=1, device_id=partner, device_id_type=MESH)

    for rb in range(8):
        rows = lax.broadcasted_iota(jnp.int32, (128, 128), 0) + rb * 128
        for g in range(8):
            onehot[0, pl.ds(rb * 128, 128), pl.ds(g * 128, 128)] = (
                (rows == ts[g : g + 1, :]).astype(jnp.float32).astype(jnp.bfloat16)
            )

    def leaving(buf, phase, order, c, there):
        dim = order[phase]
        if phase == 0:
            return (buf.at[c, there], buf.at[c, :, there], buf.at[c, :, :, there])[dim]
        if phase == 1:
            rest = sorted(order[1:])
            return buf.at[c, :, there] if rest[0] == dim else buf.at[c, :, :, there]
        return buf.at[c, :, :, there]

    def landing(buf, phase, order, c):
        dim = order[phase]
        if phase == 0:
            return buf.at[c, at[dim]]
        if phase == 1:
            seen = sorted(order[:2])
            return buf.at[c, at[dim]] if seen[0] == dim else buf.at[c, :, at[dim]]
        return (buf.at[c, at[dim]], buf.at[c, :, at[dim]], buf.at[c, :, :, at[dim]])[dim]

    bufs = (send, r1, r2, r3)
    mbufs = (ms, m1, m2, m3)

    def forward(phase, c, order, kind, ssem, rsem):
        src, dst = kind[phase], kind[phase + 1]
        dim = order[phase]
        for delta in (2, 1, 3):
            there, device = peer(dim, delta)
            pltpu.make_async_remote_copy(
                src_ref=leaving(src, phase, order, c, there),
                dst_ref=landing(dst, phase, order, c),
                send_sem=ssem, recv_sem=rsem, device_id=device, device_id_type=MESH,
            ).start()
        landing(dst, phase, order, c)[...] = leaving(src, phase, order, c, at[dim])[...]

    def take(kind, sem):
        whole = kind[0].at[0, pl.ds(0, 3)]
        pltpu.make_async_copy(whole, whole, sem).wait()

    lane_g = lax.broadcasted_iota(jnp.int32, (64, 128), 1) // CAP
    own_g = lax.broadcasted_iota(jnp.int32, (64, 128), 0) % 8
    spread = (lane_g == own_g).astype(jnp.float32)
    owner8 = lax.broadcasted_iota(jnp.int32, (8, 64), 1) // 8
    by_block = jnp.where(
        owner8 == lax.broadcasted_iota(jnp.int32, (8, 64), 0), cnts[...].astype(jnp.float32), 0.0
    )
    count = jnp.dot(by_block, spread, preferred_element_type=jnp.float32)
    lanes = lax.broadcasted_iota(jnp.int32, (8, 128), 1)
    names = jnp.concatenate([srows[:, g * 128 : g * 128 + 128] for g in range(8)], axis=0)
    names = jnp.where((lanes % CAP).astype(jnp.float32) < count, names + 1, 0)
    for j in range(8):
        turned = pltpu.roll(names, ((me % 8) - j + 8) % 8 * CAP, 1)
        turned = jnp.where(lanes // CAP == me % 8, turned, 0)
        for g in range(8):
            o = 8 * g + j
            ms[0, o // 16, (o // 4) % 4, o % 4] = turned[g : g + 1, :]

    pl.semaphore_wait(barrier, 10)
    forward(0, 0, ORDERS[0], mbufs, msend_sem.at[0], mrecv_sem.at[0])

    for c in issue:
        load(c).wait()
        send[c] = (
            jnp.dot(onehot[0], tgv[c], preferred_element_type=jnp.float32)
            .astype(jnp.bfloat16)
            .reshape(4, 4, 4, CAP, CW)
        )
        forward(0, c, ORDERS[c // PER], bufs, send_sem.at[0, c], recv_sem.at[0, c])

    take(mbufs, mrecv_sem.at[0])
    forward(1, 0, ORDERS[0], mbufs, msend_sem.at[1], mrecv_sem.at[1])
    for n, c in enumerate(issue):
        take(bufs, recv_sem.at[0, c])
        forward(1, c, ORDERS[c // PER], bufs, send_sem.at[1, c], recv_sem.at[1, c])
        if n == 2:
            take(mbufs, mrecv_sem.at[1])
            forward(2, 0, ORDERS[0], mbufs, msend_sem.at[2], mrecv_sem.at[2])
    for c in issue:
        take(bufs, recv_sem.at[1, c])
        forward(2, c, ORDERS[c // PER], bufs, send_sem.at[2, c], recv_sem.at[2, c])

    take(mbufs, mrecv_sem.at[2])
    named = m3[0].reshape(8, 8, 128).sum(axis=1)
    touched_parts = []
    for rb in range(8):
        rows = lax.broadcasted_iota(jnp.int32, (128, 128), 0) + (rb * 128 + 1)
        any_hit = jnp.zeros((128, 128), jnp.float32)
        for g in range(8):
            hit = (rows == named[g : g + 1, :]).astype(jnp.float32)
            onehot[1, pl.ds(rb * 128, 128), pl.ds(g * 128, 128)] = hit.astype(jnp.bfloat16)
            any_hit = jnp.maximum(any_hit, hit)
        touched_parts.append(jnp.max(any_hit, axis=1, keepdims=True))
    touched = to_row(jnp.concatenate(touched_parts, axis=0))
    steps = (rsteps[...] + 1).astype(jnp.float32)
    fix_first = 1.0 - jnp.exp(steps * jnp.log(jnp.float32(0.9)))
    fix_second = 1.0 - jnp.exp(steps * jnp.log(jnp.float32(0.95)))

    for n, c in enumerate(issue):
        take(bufs, recv_sem.at[2, c])
        for rb in range(8):
            part = jnp.dot(
                onehot[1, pl.ds(rb * 128, 128), :], r3[c].reshape(ROWS, CW), preferred_element_type=jnp.float32
            )
            grad[pl.ds(rb * 128, 128), pl.ds(c * CW, CW)] = part
            squares = part * part
            folded = squares[:, :128]
            for q in range(1, CW // 128):
                folded = folded + squares[:, q * 128 : q * 128 + 128]
            if n == 0:
                acc[pl.ds(rb * 128, 128), :] = folded
            else:
                acc[pl.ds(rb * 128, 128), :] += folded

    mine = to_row(jnp.sum(acc[...], axis=1, keepdims=True))
    sq_out[...] = mine
    swap = pltpu.make_async_remote_copy(
        src_ref=sq_out, dst_ref=sq_in, send_sem=sq_sem.at[0], recv_sem=sq_sem.at[1],
        device_id=partner, device_id_type=MESH,
    )
    swap.start()

    whole = send.at[0, pl.ds(0, 3)]
    for phase in range(3):
        for c in range(CHUNKS):
            pltpu.make_async_copy(whole, whole, send_sem.at[phase, c]).wait()
        pltpu.make_async_copy(ms.at[0, pl.ds(0, 3)], ms.at[0, pl.ds(0, 3)], msend_sem.at[phase]).wait()
    swap.wait()

    square = (mine + sq_in[...]) / D
    live = touched > 0.0
    second = jnp.where(live, 0.95 * rscale[...] + 0.05 * square, rscale[...])
    scale[...] = second
    denom = jnp.sqrt(second / fix_second) + 1e-08
    rate = jnp.where(live, 0.01 / (fix_first * denom), 0.0)
    keep = jnp.where(live, 0.9, 1.0)
    decay = jnp.where(live, 1.0 - 0.01 * 0.1, 1.0)
    lane = lax.broadcasted_iota(jnp.int32, (ROWS, 128), 1)
    coef[...] = jnp.where(
        lane == 0, to_column(keep), jnp.where(lane == 1, to_column(decay), to_column(rate))
    )


def update(grad, coef, weights, moment, new_weights, new_moment):
    keep = coef[:, 0:1]
    decay = coef[:, 1:2]
    rate = coef[:, 2:3]
    first = keep * moment[...].astype(jnp.float32) + 0.1 * grad[...]
    new_moment[...] = first.astype(jnp.bfloat16)
    new_weights[...] = (decay * weights[...].astype(jnp.float32) - rate * first).astype(jnp.bfloat16)


def shards(token_grads, token_slot, slot_rows, counts, weights, moment, row_scale, row_steps):
    vmem = pl.BlockSpec(memory_space=pltpu.VMEM)
    block = (4, 4, 4, CAP, CW)
    bf16, f32, i32 = jnp.bfloat16, jnp.float32, jnp.int32
    grad, coef, scale = pl.pallas_call(
        exchange,
        name="exchange",
        out_shape=(
            jax.ShapeDtypeStruct((ROWS, HALF), f32),
            jax.ShapeDtypeStruct((ROWS, 128), f32),
            jax.ShapeDtypeStruct((8, 128), f32),
        ),
        in_specs=[pl.BlockSpec(memory_space=pl.ANY)] + [vmem] * 5,
        out_specs=(vmem, vmem, vmem),
        scratch_shapes=[
            pltpu.VMEM((CHUNKS, ROWS, CW), bf16),
            pltpu.VMEM((CHUNKS,) + block, bf16),
            pltpu.VMEM((CHUNKS,) + block, bf16),
            pltpu.VMEM((CHUNKS,) + block, bf16),
            pltpu.VMEM((CHUNKS,) + block, bf16),
            pltpu.VMEM((2, ROWS, ROWS), bf16),
            pltpu.VMEM((1, 4, 4, 4, 1, 128), i32),
            pltpu.VMEM((1, 4, 4, 4, 1, 128), i32),
            pltpu.VMEM((1, 4, 4, 4, 1, 128), i32),
            pltpu.VMEM((1, 4, 4, 4, 1, 128), i32),
            pltpu.VMEM((ROWS, 128), f32),
            pltpu.VMEM((8, 128), f32),
            pltpu.VMEM((8, 128), f32),
            pltpu.SemaphoreType.DMA((CHUNKS,)),
            pltpu.SemaphoreType.DMA((3, CHUNKS)),
            pltpu.SemaphoreType.DMA((3, CHUNKS)),
            pltpu.SemaphoreType.DMA((3,)),
            pltpu.SemaphoreType.DMA((3,)),
            pltpu.SemaphoreType.DMA((2,)),
        ],
        compiler_params=pltpu.CompilerParams(
            collective_id=0, has_side_effects=True, vmem_limit_bytes=48 * 1024 * 1024
        ),
        cost_estimate=pl.CostEstimate(flops=10**10, bytes_accessed=2 * 10**7, transcendentals=0),
    )(
        token_grads, token_slot.reshape(8, 128), slot_rows, counts,
        row_scale.reshape(8, 128), row_steps.reshape(8, 128),
    )
    tall = 128
    wide = pl.BlockSpec((tall, HALF), lambda i: (i, 0))
    new_weights, new_moment = pl.pallas_call(
        update,
        name="update",
        grid=(ROWS // tall,),
        out_shape=(jax.ShapeDtypeStruct((ROWS, HALF), bf16), jax.ShapeDtypeStruct((ROWS, HALF), bf16)),
        in_specs=[wide, pl.BlockSpec((tall, 128), lambda i: (i, 0)), wide, wide],
        out_specs=(wide, wide),
        cost_estimate=pl.CostEstimate(flops=2 * 10**7, bytes_accessed=3 * 10**7, transcendentals=0),
    )(grad, coef, weights, moment)
    return (new_weights, new_moment, scale.reshape(ROWS))


def solution(mesh):
    return jax.shard_map(
        shards,
        mesh=mesh,
        in_specs=(
            P("vocab", "width"),
            P("vocab"),
            P("vocab", None),
            P("vocab", None),
            P("vocab", "width"),
            P("vocab", "width"),
            P("vocab"),
            P("vocab"),
        ),
        out_specs=(P("vocab", "width"), P("vocab", "width"), P("vocab")),
        check_vma=False,
    )
```

```python
import functools
import jax
import jax.numpy as jnp
from jax import lax
from jax.experimental import pallas as pl
from jax.experimental.pallas import tpu as pltpu
from jax.sharding import PartitionSpec as P

D = 4608
HALF = 2304
ROWS = 1024
CAP = 16
GROUPS = 3
WIDTHS = (128, 256, 256, 128)
PER = len(WIDTHS)
CHUNKS = GROUPS * PER
WIDTH = WIDTHS * GROUPS
FIRST = tuple(sum(WIDTH[:c]) for c in range(CHUNKS))
TALL = 128
MESH = pl.DeviceIdType.MESH
ORDERS = ((0, 1, 2), (1, 2, 0), (2, 0, 1))


def to_row(column):
    eye = lax.broadcasted_iota(jnp.int32, (128, 128), 0) == lax.broadcasted_iota(jnp.int32, (128, 128), 1)
    parts = [
        jnp.sum(jnp.where(eye, column[g * 128 : g * 128 + 128, :], 0.0), axis=0, keepdims=True)
        for g in range(8)
    ]
    return jnp.concatenate(parts, axis=0)


def exchange(
    tg, ts_hbm, srows_hbm, cnts_hbm, rscale_hbm, rsteps_hbm, weights, moment,
    first, coef, scale, weights_v,
    ts, srows, cnts, rscale, rsteps, moment_v, keep,
    tgv, send, r1, r2, r3, onehot, ms, m1, m2, m3, acc, sq_out, sq_in,
    small_sem, wide_sem, load_sem, send_sem, recv_sem, msend_sem, mrecv_sem, sq_sem,
):
    me = lax.axis_index("vocab")
    core = lax.axis_index("width")
    at = (me // 16, (me // 4) % 4, me % 4)
    stride = (16, 4, 1)

    def peer(dim, delta):
        there = (at[dim] + delta) % 4
        return there, (me + (there - at[dim]) * stride[dim], core)

    def load(c):
        return pltpu.make_async_copy(tg.at[:, pl.ds(FIRST[c], WIDTH[c])], tgv[c], load_sem.at[c])

    issue = [g * PER + k for k in range(PER) for g in range(GROUPS)]
    small = [
        pltpu.make_async_copy(src, dst, small_sem.at[i])
        for i, (src, dst) in enumerate(
            ((ts_hbm, ts), (srows_hbm, srows), (cnts_hbm, cnts), (rscale_hbm, rscale), (rsteps_hbm, rsteps))
        )
    ]
    for copy in small:
        copy.start()
    for c in issue:
        load(c).start()
    wide = [
        pltpu.make_async_copy(src, dst, wide_sem.at[i])
        for i, (src, dst) in enumerate(((weights, weights_v), (moment, moment_v)))
    ]

    barrier = pltpu.get_barrier_semaphore()
    for dim in range(3):
        for delta in (1, 2, 3):
            pl.semaphore_signal(barrier, inc=1, device_id=peer(dim, delta)[1], device_id_type=MESH)
    partner = (me, 1 - core)
    pl.semaphore_signal(barrier, inc=1, device_id=partner, device_id_type=MESH)

    for copy in small:
        copy.wait()
    for rb in range(8):
        rows = lax.broadcasted_iota(jnp.int32, (128, 128), 0) + rb * 128
        for g in range(8):
            onehot[0, pl.ds(rb * 128, 128), pl.ds(g * 128, 128)] = (
                (rows == ts[g : g + 1, :]).astype(jnp.float32).astype(jnp.bfloat16)
            )

    def leaving(buf, phase, order, c, there):
        dim = order[phase]
        if phase == 0:
            return (buf[c].at[there], buf[c].at[:, there], buf[c].at[:, :, there])[dim]
        if phase == 1:
            rest = sorted(order[1:])
            return buf[c].at[:, there] if rest[0] == dim else buf[c].at[:, :, there]
        return buf[c].at[:, :, there]

    def landing(buf, phase, order, c):
        dim = order[phase]
        if phase == 0:
            return buf[c].at[at[dim]]
        if phase == 1:
            seen = sorted(order[:2])
            return buf[c].at[at[dim]] if seen[0] == dim else buf[c].at[:, at[dim]]
        return (buf[c].at[at[dim]], buf[c].at[:, at[dim]], buf[c].at[:, :, at[dim]])[dim]

    bufs = (send, r1, r2, r3)
    mbufs = ((ms,), (m1,), (m2,), (m3,))

    def forward(phase, c, order, kind, ssem, rsem):
        src, dst = kind[phase], kind[phase + 1]
        dim = order[phase]
        for delta in (2, 1, 3):
            there, device = peer(dim, delta)
            pltpu.make_async_remote_copy(
                src_ref=leaving(src, phase, order, c, there),
                dst_ref=landing(dst, phase, order, c),
                send_sem=ssem, recv_sem=rsem, device_id=device, device_id_type=MESH,
            ).start()
        landing(dst, phase, order, c)[...] = leaving(src, phase, order, c, at[dim])[...]

    def take(kind, c, sem):
        whole = kind[0][c].at[pl.ds(0, 3)]
        pltpu.make_async_copy(whole, whole, sem).wait()

    lane_g = lax.broadcasted_iota(jnp.int32, (64, 128), 1) // CAP
    own_g = lax.broadcasted_iota(jnp.int32, (64, 128), 0) % 8
    spread = (lane_g == own_g).astype(jnp.float32)
    owner8 = lax.broadcasted_iota(jnp.int32, (8, 64), 1) // 8
    by_block = jnp.where(
        owner8 == lax.broadcasted_iota(jnp.int32, (8, 64), 0), cnts[...].astype(jnp.float32), 0.0
    )
    count = jnp.dot(by_block, spread, preferred_element_type=jnp.float32)
    lanes = lax.broadcasted_iota(jnp.int32, (8, 128), 1)
    names = jnp.concatenate([srows[:, g * 128 : g * 128 + 128] for g in range(8)], axis=0)
    names = jnp.where((lanes % CAP).astype(jnp.float32) < count, names + 1, 0)
    for j in range(8):
        turned = pltpu.roll(names, ((me % 8) - j + 8) % 8 * CAP, 1)
        turned = jnp.where(lanes // CAP == me % 8, turned, 0)
        for g in range(8):
            o = 8 * g + j
            ms[o // 16, (o // 4) % 4, o % 4] = turned[g : g + 1, :]

    pl.semaphore_wait(barrier, 10)
    forward(0, 0, ORDERS[0], mbufs, msend_sem.at[0], mrecv_sem.at[0])

    for c in issue:
        load(c).wait()
        send[c][...] = (
            jnp.dot(onehot[0], tgv[c][...], preferred_element_type=jnp.float32)
            .astype(jnp.bfloat16)
            .reshape(4, 4, 4, CAP, WIDTH[c])
        )
        forward(0, c, ORDERS[c // PER], bufs, send_sem.at[0, c], recv_sem.at[0, c])

    for copy in wide:
        copy.start()
    take(mbufs, 0, mrecv_sem.at[0])
    forward(1, 0, ORDERS[0], mbufs, msend_sem.at[1], mrecv_sem.at[1])
    for n, c in enumerate(issue):
        take(bufs, c, recv_sem.at[0, c])
        forward(1, c, ORDERS[c // PER], bufs, send_sem.at[1, c], recv_sem.at[1, c])
        if n == 2:
            take(mbufs, 0, mrecv_sem.at[1])
            forward(2, 0, ORDERS[0], mbufs, msend_sem.at[2], mrecv_sem.at[2])
    for c in issue:
        take(bufs, c, recv_sem.at[1, c])
        forward(2, c, ORDERS[c // PER], bufs, send_sem.at[2, c], recv_sem.at[2, c])

    take(mbufs, 0, mrecv_sem.at[2])
    named = m3[...].reshape(8, 8, 128).sum(axis=1)
    touched_parts = []
    for rb in range(8):
        rows = lax.broadcasted_iota(jnp.int32, (128, 128), 0) + (rb * 128 + 1)
        any_hit = jnp.zeros((128, 128), jnp.float32)
        for g in range(8):
            hit = (rows == named[g : g + 1, :]).astype(jnp.float32)
            onehot[1, pl.ds(rb * 128, 128), pl.ds(g * 128, 128)] = hit.astype(jnp.bfloat16)
            any_hit = jnp.maximum(any_hit, hit)
        hit_column = jnp.max(any_hit, axis=1, keepdims=True)
        touched_parts.append(hit_column)
        keep[pl.ds(rb * 128, 128), :] = jnp.broadcast_to(1.0 - 0.1 * hit_column, (128, 128))
    touched = to_row(jnp.concatenate(touched_parts, axis=0))
    steps = (rsteps[...] + 1).astype(jnp.float32)
    fix_first = 1.0 - jnp.exp(steps * jnp.log(jnp.float32(0.9)))
    fix_second = 1.0 - jnp.exp(steps * jnp.log(jnp.float32(0.95)))

    for copy in wide:
        copy.wait()
    for n, c in enumerate(issue):
        take(bufs, c, recv_sem.at[2, c])
        received = r3[c][...].reshape(ROWS, WIDTH[c])
        for rb in range(8):
            rows = pl.ds(rb * 128, 128)
            part = jnp.dot(onehot[1, rows, :], received, preferred_element_type=jnp.float32)
            folded = None
            for q in range(0, WIDTH[c], 128):
                columns = pl.ds(FIRST[c] + q, 128)
                piece = part[:, q : q + 128]
                first[rows, columns] = (
                    keep[rows, :] * moment_v[rows, columns].astype(jnp.float32) + 0.1 * piece
                )
                folded = piece * piece if folded is None else folded + piece * piece
            if n == 0:
                acc[rows, :] = folded
            else:
                acc[rows, :] += folded

    mine = to_row(jnp.sum(acc[...], axis=1, keepdims=True))
    sq_out[...] = mine
    swap = pltpu.make_async_remote_copy(
        src_ref=sq_out, dst_ref=sq_in, send_sem=sq_sem.at[0], recv_sem=sq_sem.at[1],
        device_id=partner, device_id_type=MESH,
    )
    swap.start()

    for phase in range(3):
        for c in range(CHUNKS):
            take(bufs, c, send_sem.at[phase, c])
        take(mbufs, 0, msend_sem.at[phase])
    swap.wait()

    square = (mine + sq_in[...]) / D
    live = touched > 0.0
    second = jnp.where(live, 0.95 * rscale[...] + 0.05 * square, rscale[...])
    scale[...] = second
    denom = jnp.sqrt(second / fix_second) + 1e-08
    rate = jnp.where(live, 0.01 / (fix_first * denom), 0.0)
    decay = jnp.where(live, 1.0 - 0.01 * 0.1, 1.0)
    eye = lax.broadcasted_iota(jnp.int32, (128, 128), 0) == lax.broadcasted_iota(jnp.int32, (128, 128), 1)
    for g in range(8):
        for i, value in enumerate((decay, rate)):
            column = jnp.sum(jnp.where(eye, value[g : g + 1, :], 0.0), axis=1, keepdims=True)
            coef[i, pl.ds(g * 128, 128), :] = jnp.broadcast_to(column, (128, 128))


def update(first, coef, scale, weights, new_weights, new_moment, new_scale):
    new_scale[...] = scale[...]
    for r in range(0, TALL, 16):
        rows = pl.ds(r, 16)
        decay, rate = coef[0, rows, :], coef[1, rows, :]
        for q in range(0, HALF, 128):
            columns = pl.ds(q, 128)
            value = first[rows, columns]
            new_moment[rows, columns] = value.astype(jnp.bfloat16)
            old = weights[rows, columns].astype(jnp.float32)
            new_weights[rows, columns] = (decay * old - rate * value).astype(jnp.bfloat16)


def shards(token_grads, token_slot, slot_rows, counts, weights, moment, row_scale, row_steps):
    vmem = pl.BlockSpec(memory_space=pltpu.VMEM)
    hbm = pl.BlockSpec(memory_space=pltpu.HBM)
    bf16, f32, i32 = jnp.bfloat16, jnp.float32, jnp.int32
    blocks = tuple(pltpu.VMEM((4, 4, 4, CAP, w), bf16) for w in WIDTH)
    first, coef, scale, weights_v = pl.pallas_call(
        exchange,
        name="exchange",
        out_shape=(
            pltpu.VMEM((ROWS, HALF), f32),
            pltpu.VMEM((2, ROWS, 128), f32),
            pltpu.VMEM((8, 128), f32),
            pltpu.VMEM((ROWS, HALF), bf16),
        ),
        in_specs=[hbm] * 8,
        out_specs=(vmem,) * 4,
        scratch_shapes=[
            pltpu.VMEM((8, 128), i32),
            pltpu.VMEM((1, 1024), i32),
            pltpu.VMEM((1, 64), i32),
            pltpu.VMEM((8, 128), f32),
            pltpu.VMEM((8, 128), i32),
            pltpu.VMEM((ROWS, HALF), bf16),
            pltpu.VMEM((ROWS, 128), f32),
            tuple(pltpu.VMEM((ROWS, w), bf16) for w in WIDTH),
            blocks, blocks, blocks, blocks,
            pltpu.VMEM((2, ROWS, ROWS), bf16),
            pltpu.VMEM((4, 4, 4, 1, 128), i32),
            pltpu.VMEM((4, 4, 4, 1, 128), i32),
            pltpu.VMEM((4, 4, 4, 1, 128), i32),
            pltpu.VMEM((4, 4, 4, 1, 128), i32),
            pltpu.VMEM((ROWS, 128), f32),
            pltpu.VMEM((8, 128), f32),
            pltpu.VMEM((8, 128), f32),
            pltpu.SemaphoreType.DMA((5,)),
            pltpu.SemaphoreType.DMA((2,)),
            pltpu.SemaphoreType.DMA((CHUNKS,)),
            pltpu.SemaphoreType.DMA((3, CHUNKS)),
            pltpu.SemaphoreType.DMA((3, CHUNKS)),
            pltpu.SemaphoreType.DMA((3,)),
            pltpu.SemaphoreType.DMA((3,)),
            pltpu.SemaphoreType.DMA((2,)),
        ],
        compiler_params=pltpu.CompilerParams(
            collective_id=0, has_side_effects=True, vmem_limit_bytes=38 * 1024 * 1024
        ),
        cost_estimate=pl.CostEstimate(flops=10**10, bytes_accessed=2 * 10**7, transcendentals=0),
    )(*(
        pltpu.with_memory_space_constraint(value, pltpu.HBM)
        for value in (
            token_grads, token_slot.reshape(8, 128), slot_rows, counts,
            row_scale.reshape(8, 128), row_steps.reshape(8, 128), weights, moment,
        )
    ))
    wide = pl.BlockSpec((TALL, HALF), lambda i: (i, 0))
    row = pl.BlockSpec((8, 128), lambda i: (0, 0))
    new_weights, new_moment, new_scale = pl.pallas_call(
        update,
        name="update",
        grid=(ROWS // TALL,),
        out_shape=(
            jax.ShapeDtypeStruct((ROWS, HALF), bf16),
            jax.ShapeDtypeStruct((ROWS, HALF), bf16),
            jax.ShapeDtypeStruct((8, 128), f32),
        ),
        in_specs=[wide, pl.BlockSpec((2, TALL, 128), lambda i: (0, i, 0)), row, wide],
        out_specs=(wide, wide, row),
        compiler_params=pltpu.CompilerParams(vmem_limit_bytes=10 * 1024 * 1024),
        cost_estimate=pl.CostEstimate(flops=2 * 10**7, bytes_accessed=3 * 10**7, transcendentals=0),
    )(first, coef, scale, weights_v)
    return (new_weights, new_moment, new_scale.reshape(ROWS))


def solution(mesh):
    return jax.shard_map(
        shards,
        mesh=mesh,
        in_specs=(
            P("vocab", "width"),
            P("vocab"),
            P("vocab", None),
            P("vocab", None),
            P("vocab", "width"),
            P("vocab", "width"),
            P("vocab"),
            P("vocab"),
        ),
        out_specs=(P("vocab", "width"), P("vocab", "width"), P("vocab")),
        check_vma=False,
    )
```

```python
import functools
import jax
import jax.numpy as jnp
from jax import lax
from jax.experimental import pallas as pl
from jax.experimental.pallas import tpu as pltpu
from jax.sharding import PartitionSpec as P

D = 4608
HALF = 2304
ROWS = 1024
CAP = 16
PLANE = 128
LINE = 208
GROUPS = 3
WIDTHS = (256, 256, 256)
PER = len(WIDTHS)
CHUNKS = GROUPS * PER
WIDTH = WIDTHS * GROUPS
FIRST = tuple(sum(WIDTH[:c]) for c in range(CHUNKS))
TALL = 128
MESH = pl.DeviceIdType.MESH
ORDERS = ((0, 1, 2), (1, 2, 0), (2, 0, 1))


def to_row(column):
    eye = lax.broadcasted_iota(jnp.int32, (128, 128), 0) == lax.broadcasted_iota(jnp.int32, (128, 128), 1)
    parts = [
        jnp.sum(jnp.where(eye, column[g * 128 : g * 128 + 128, :], 0.0), axis=0, keepdims=True)
        for g in range(8)
    ]
    return jnp.concatenate(parts, axis=0)


def exchange(
    tg, ts_hbm, srows_hbm, cnts_hbm, rscale_hbm, rsteps_hbm, weights, moment,
    first, coef, scale, weights_v, over,
    ts, srows, cnts, rscale, rsteps, keep,
    tgv, s0, r1, s1, r2, s2, r3, onehot, place, pack, unpack, pbuf,
    ct1, ct2, flags, ms, m1, m2, m3, acc, sq_out, sq_in,
    small_sem, wide_sem, load_sem, moment_sem, send_sem, recv_sem, msend_sem, mrecv_sem, sq_sem,
    ct_sem, flag_sem,
):
    me = lax.axis_index("vocab")
    core = lax.axis_index("width")
    at = (me // 16, (me // 4) % 4, me % 4)
    stride = (16, 4, 1)

    def peer(dim, delta):
        there = (at[dim] + delta) % 4
        return there, (me + (there - at[dim]) * stride[dim], core)

    def load(c):
        return pltpu.make_async_copy(tg.at[:, pl.ds(FIRST[c], WIDTH[c])], tgv[c], load_sem.at[c])

    issue = [g * PER + k for k in range(PER) for g in range(GROUPS)]
    small = [
        pltpu.make_async_copy(src, dst, small_sem.at[i])
        for i, (src, dst) in enumerate(
            ((ts_hbm, ts), (srows_hbm, srows), (cnts_hbm, cnts), (rscale_hbm, rscale), (rsteps_hbm, rsteps))
        )
    ]
    for copy in small:
        copy.start()
    for c in issue:
        load(c).start()
    wide = pltpu.make_async_copy(weights, weights_v, wide_sem)

    def load_moment(c):
        return pltpu.make_async_copy(
            moment.at[:, pl.ds(FIRST[c], WIDTH[c])], tgv[c], moment_sem.at[c]
        )

    barrier = pltpu.get_barrier_semaphore()
    for dim in range(3):
        for delta in (1, 2, 3):
            pl.semaphore_signal(barrier, inc=1, device_id=peer(dim, delta)[1], device_id_type=MESH)
    partner = (me, 1 - core)
    pl.semaphore_signal(barrier, inc=1, device_id=partner, device_id_type=MESH)

    for copy in small:
        copy.wait()
    for rb in range(8):
        rows = lax.broadcasted_iota(jnp.int32, (128, 128), 0) + rb * 128
        for g in range(8):
            onehot[pl.ds(rb * 128, 128), pl.ds(g * 128, 128)] = (
                (rows == ts[g : g + 1, :]).astype(jnp.float32).astype(jnp.bfloat16)
            )

    def names_part(buf, phase, there):
        if phase == 0:
            return buf.at[there]
        return buf.at[:, there] if phase == 1 else buf.at[:, :, there]

    def post(src_of, dst, dim, ssem, rsem, own=True):
        for delta in (2, 1, 3):
            there, device = peer(dim, delta)
            pltpu.make_async_remote_copy(
                src_ref=src_of(there), dst_ref=dst,
                send_sem=ssem, recv_sem=rsem, device_id=device, device_id_type=MESH,
            ).start()
        if own:
            dst[...] = src_of(at[dim])[...]

    def post_names(phase):
        bufs = (ms, m1, m2, m3)
        post(
            lambda there: names_part(bufs[phase], phase, there),
            names_part(bufs[phase + 1], phase, at[phase]),
            phase, msend_sem.at[phase], mrecv_sem.at[phase],
        )

    def post_rows(phase, c):
        order = ORDERS[c // PER]
        dim = order[phase]
        src, dst = ((s0, r1), (s1, r2), (s2, r3))[phase]
        if phase < 2:
            target = dst[c].at[at[dim]]
        else:
            target = (dst[c].at[at[dim]], dst[c].at[:, at[dim]], dst[c].at[:, :, at[dim]])[dim]
        post(lambda there: src[c].at[there], target, dim, send_sem.at[phase, c], recv_sem.at[phase, c])

    def take(blocks, sem):
        whole = blocks.at[pl.ds(0, 3)]
        pltpu.make_async_copy(whole, whole, sem).wait()

    staged = (s0, s1, s2)

    def take_rows(phase, c):
        take(staged[phase][c], recv_sem.at[phase, c])

    def coordinate(owner, dim):
        return (owner // stride[dim]) % 4

    lane_g = lax.broadcasted_iota(jnp.int32, (64, 128), 1) // CAP
    own_g = lax.broadcasted_iota(jnp.int32, (64, 128), 0) % 8
    spread = (lane_g == own_g).astype(jnp.float32)
    owner8 = lax.broadcasted_iota(jnp.int32, (8, 64), 1) // 8
    by_block = jnp.where(
        owner8 == lax.broadcasted_iota(jnp.int32, (8, 64), 0), cnts[...].astype(jnp.float32), 0.0
    )
    count = jnp.dot(by_block, spread, preferred_element_type=jnp.float32)
    lanes = lax.broadcasted_iota(jnp.int32, (8, 128), 1)
    names = jnp.concatenate([srows[:, g * 128 : g * 128 + 128] for g in range(8)], axis=0)
    names = jnp.where((lanes % CAP).astype(jnp.float32) < count, names + 1, 0)
    for j in range(8):
        turned = pltpu.roll(names, ((me % 8) - j + 8) % 8 * CAP, 1)
        turned = jnp.where(lanes // CAP == me % 8, turned, 0)
        for g in range(8):
            o = 8 * g + j
            ms[o // 16, (o // 4) % 4, o % 4] = turned[g : g + 1, :]


    cnt8 = jnp.broadcast_to(cnts[...].astype(jnp.float32), (8, 64))
    o_from = lax.broadcasted_iota(jnp.int32, (64, 64), 0)
    o_to = lax.broadcasted_iota(jnp.int32, (64, 64), 1)
    o_slot = lax.broadcasted_iota(jnp.int32, (8, 128), 0) * 8 + lanes // CAP
    excess = jnp.zeros((8, 64), jnp.float32)
    for g, (a, b, c) in enumerate(ORDERS):
        same = coordinate(o_from, a) == coordinate(o_to, a)
        ahead = same & (
            coordinate(o_from, b) * 4 + coordinate(o_from, c)
            < coordinate(o_to, b) * 4 + coordinate(o_to, c)
        )
        before = jnp.dot(cnt8, ahead.astype(jnp.float32), preferred_element_type=jnp.float32)
        total = jnp.dot(cnt8, same.astype(jnp.float32), preferred_element_type=jnp.float32)
        excess = jnp.maximum(excess, total - PLANE)
        before = jnp.where(owner8 == lax.broadcasted_iota(jnp.int32, (8, 64), 0), before, 0.0)
        before = jnp.dot(before, spread, preferred_element_type=jnp.float32)
        place_at = (coordinate(o_slot, a) * PLANE + lanes % CAP).astype(jnp.float32) + before
        high = jnp.floor(place_at * (1.0 / 32.0))
        low = place_at - 32.0 * high
        for blk in range(8):
            pbuf[blk, pl.ds(2 * g, 1), :] = high[blk : blk + 1, :]
            pbuf[blk, pl.ds(2 * g + 1, 1), :] = low[blk : blk + 1, :]
    for blk in range(8):
        pbuf[blk, pl.ds(6, 2), :] = jnp.zeros((2, 128), jnp.float32)
    token_at = jnp.zeros((8, ROWS), jnp.float32)
    for blk in range(8):
        token_at = token_at + jnp.dot(
            pbuf[blk].astype(jnp.bfloat16), onehot[pl.ds(blk * 128, 128), :],
            preferred_element_type=jnp.float32,
        )
    for g in range(GROUPS):
        where_to = 32.0 * token_at[2 * g : 2 * g + 1, :] + token_at[2 * g + 1 : 2 * g + 2, :]
        for rb in range(0, 4 * PLANE, 128):
            rows = (lax.broadcasted_iota(jnp.int32, (128, ROWS), 0) + rb).astype(jnp.float32)
            place[g, pl.ds(rb, 128), :] = (rows == where_to).astype(jnp.float32).astype(jnp.bfloat16)

    pl.semaphore_wait(barrier, 10)
    for dim in range(3):
        post(lambda there: cnts, ct1.at[dim, at[dim]], dim, ct_sem.at[0, dim], ct_sem.at[1, dim])
    post_names(0)

    for c in issue:
        load(c).wait()
        s0[c][...] = (
            jnp.dot(place[c // PER], tgv[c][...], preferred_element_type=jnp.float32)
            .astype(jnp.bfloat16)
            .reshape(4, PLANE, WIDTH[c])
        )
        post_rows(0, c)

    b_of = lax.broadcasted_iota(jnp.int32, (8, 64), 0)
    o_line = lax.broadcasted_iota(jnp.int32, (8, 64), 1)
    ones = jnp.ones((64, 128), jnp.float32)
    excess = jnp.max(jnp.max(excess, axis=1, keepdims=True), axis=0, keepdims=True)
    idx = lanes.astype(jnp.float32)
    line_at = (lax.broadcasted_iota(jnp.int32, (8, 128), 0) * LINE).astype(jnp.float32)
    for dim in range(3):
        take(ct1.at[dim], ct_sem.at[1, dim])
    for g, (a, b, c) in enumerate(ORDERS):
        post(
            lambda there: ct1.at[a], ct2.at[g, at[b]], b, ct_sem.at[2, g], ct_sem.at[3, g]
        )
        in_plane = coordinate(o_line, a) == at[a]
        b_owner = coordinate(o_line, b)
        base = jnp.zeros((8, 128), jnp.float32)
        for source in range(4):
            row = jnp.broadcast_to(ct1[a, source].astype(jnp.float32), (8, 64))
            offset = jnp.dot(
                jnp.where(in_plane & (b_owner < b_of), row, 0.0), ones, preferred_element_type=jnp.float32
            )
            length = jnp.dot(
                jnp.where(in_plane & (b_owner == b_of), row, 0.0), ones, preferred_element_type=jnp.float32
            )
            inside = (idx >= offset) & (idx < offset + length)
            goes = jnp.sum(
                jnp.where(inside, line_at + base + idx - offset + 1.0, 0.0), axis=0, keepdims=True
            )
            for rb in range(0, 4 * LINE, 208):
                rows = (lax.broadcasted_iota(jnp.int32, (208, 128), 0) + (rb + 1)).astype(jnp.float32)
                pack[g, pl.ds(rb, 208), pl.ds(source * 128, 128)] = (
                    (rows == goes).astype(jnp.float32).astype(jnp.bfloat16)
                )
            base = base + length
        most = jnp.max(base - LINE, axis=0, keepdims=True)
        excess = jnp.maximum(excess, most)
    flags[0, at[0]] = jnp.where(excess > 0.0, 1, 0)

    def post_flag(dim):
        post(
            lambda there: flags.at[dim, at[dim]], flags.at[dim, at[dim]], dim,
            flag_sem.at[0, dim], flag_sem.at[1, dim], own=False,
        )

    take(m1, mrecv_sem.at[0])
    post_names(1)
    for n, c in enumerate(issue):
        take_rows(0, c)
        s1[c][...] = (
            jnp.dot(pack[c // PER], r1[c][...].reshape(4 * PLANE, WIDTH[c]), preferred_element_type=jnp.float32)
            .astype(jnp.bfloat16)
            .reshape(4, LINE, WIDTH[c])
        )
        post_rows(1, c)
        load_moment(c).start()
        if n == 0:
            post_flag(0)
        if n == 2:
            take(m1, mrecv_sem.at[1])
            post_names(2)
            take(flags.at[0], flag_sem.at[1, 0])
            flags[1, at[1]] = jnp.max(flags[0], axis=0)
        if n == 3:
            post_flag(1)
        if n == 5:
            take(flags.at[1], flag_sem.at[1, 1])
            flags[2, at[2]] = jnp.max(flags[1], axis=0)
        if n == 6:
            post_flag(2)
    wide.start()

    unit = lax.broadcasted_iota(jnp.int32, (64, 64), 0)
    slot_unit = (
        lax.broadcasted_iota(jnp.int32, (ROWS, 64), 0) // CAP == lax.broadcasted_iota(jnp.int32, (ROWS, 64), 1)
    ).astype(jnp.float32)
    slot = lax.broadcasted_iota(jnp.int32, (ROWS, 128), 0)
    for g, (a, b, c) in enumerate(ORDERS):
        take(ct2.at[g], ct_sem.at[3, g])
        c_unit = unit // 16
        a_unit, b_unit = ((unit // 4) % 4, unit % 4) if a < b else (unit % 4, (unit // 4) % 4)
        in_line = (coordinate(o_to, a) == at[a]) & (coordinate(o_to, b) == at[b])
        c_owner = coordinate(o_to, c)
        begin = jnp.zeros((64, 64), jnp.float32)
        size = jnp.zeros((64, 64), jnp.float32)
        for sb in range(4):
            for sa in range(4):
                row = jnp.broadcast_to(ct2[g, sb, sa].astype(jnp.float32), (64, 64))
                row = jnp.where(in_line & (b_unit == sb), row, 0.0)
                begin = begin + jnp.where(
                    (a_unit > sa) | ((a_unit == sa) & (c_owner < c_unit)), row, 0.0
                )
                size = size + jnp.where((a_unit == sa) & (c_owner == c_unit), row, 0.0)
        begin = jnp.dot(begin, ones, preferred_element_type=jnp.float32)
        size = jnp.dot(size, ones, preferred_element_type=jnp.float32)
        begin = jnp.dot(slot_unit, begin, preferred_element_type=jnp.float32)
        size = jnp.dot(slot_unit, size, preferred_element_type=jnp.float32)
        within = (slot % CAP).astype(jnp.float32)
        sb_slot = (slot // CAP) % 4 if a < b else (slot // (CAP * 4)) % 4
        comes = jnp.where(
            within < size, (sb_slot * LINE).astype(jnp.float32) + begin + within, -1.0
        )
        for q in range(0, 4 * LINE, 128):
            span = min(128, 4 * LINE - q)
            columns = (lax.broadcasted_iota(jnp.int32, (ROWS, span), 1) + q).astype(jnp.float32)
            unpack[g, :, pl.ds(q, span)] = (
                (columns == comes[:, :span]).astype(jnp.float32).astype(jnp.bfloat16)
            )

    for c in issue:
        take_rows(1, c)
        s2[c][...] = (
            jnp.dot(unpack[c // PER], r2[c][...].reshape(4 * LINE, WIDTH[c]), preferred_element_type=jnp.float32)
            .astype(jnp.bfloat16)
            .reshape(4, 4, 4, CAP, WIDTH[c])
        )
        post_rows(2, c)

    take(m1, mrecv_sem.at[2])
    named = m3[...].reshape(8, 8, 128).sum(axis=1)
    touched_parts = []
    for rb in range(8):
        rows = lax.broadcasted_iota(jnp.int32, (128, 128), 0) + (rb * 128 + 1)
        any_hit = jnp.zeros((128, 128), jnp.float32)
        for g in range(8):
            hit = (rows == named[g : g + 1, :]).astype(jnp.float32)
            onehot[pl.ds(rb * 128, 128), pl.ds(g * 128, 128)] = hit.astype(jnp.bfloat16)
            any_hit = jnp.maximum(any_hit, hit)
        hit_column = jnp.max(any_hit, axis=1, keepdims=True)
        touched_parts.append(hit_column)
        keep[pl.ds(rb * 128, 128), :] = jnp.broadcast_to(1.0 - 0.1 * hit_column, (128, 128))
    touched = to_row(jnp.concatenate(touched_parts, axis=0))
    steps = (rsteps[...] + 1).astype(jnp.float32)
    fix_first = 1.0 - jnp.exp(steps * jnp.log(jnp.float32(0.9)))
    fix_second = 1.0 - jnp.exp(steps * jnp.log(jnp.float32(0.95)))

    for n, c in enumerate(issue):
        take_rows(2, c)
        load_moment(c).wait()
        received = r3[c][...].reshape(ROWS, WIDTH[c])
        for rb in range(8):
            rows = pl.ds(rb * 128, 128)
            part = jnp.dot(onehot[rows, :], received, preferred_element_type=jnp.float32)
            folded = None
            for q in range(0, WIDTH[c], 128):
                columns = pl.ds(FIRST[c] + q, 128)
                piece = part[:, q : q + 128]
                first[rows, columns] = (
                    keep[rows, :] * tgv[c][rows, pl.ds(q, 128)].astype(jnp.float32) + 0.1 * piece
                )
                folded = piece * piece if folded is None else folded + piece * piece
            if n == 0:
                acc[rows, :] = folded
            else:
                acc[rows, :] += folded

    mine = to_row(jnp.sum(acc[...], axis=1, keepdims=True))
    sq_out[...] = mine
    swap = pltpu.make_async_remote_copy(
        src_ref=sq_out, dst_ref=sq_in, send_sem=sq_sem.at[0], recv_sem=sq_sem.at[1],
        device_id=partner, device_id_type=MESH,
    )
    swap.start()

    for phase in range(3):
        for c in range(CHUNKS):
            take(staged[phase][c], send_sem.at[phase, c])
        take(m1, msend_sem.at[phase])
        take(ct1.at[0], ct_sem.at[0, phase])
        take(ct2.at[0], ct_sem.at[2, phase])
        take(flags.at[0], flag_sem.at[0, phase])
    take(flags.at[2], flag_sem.at[1, 2])
    over[...] = jnp.max(flags[2], axis=0)
    wide.wait()
    swap.wait()

    square = (mine + sq_in[...]) / D
    live = touched > 0.0
    second = jnp.where(live, 0.95 * rscale[...] + 0.05 * square, rscale[...])
    scale[...] = second
    denom = jnp.sqrt(second / fix_second) + 1e-08
    rate = jnp.where(live, 0.01 / (fix_first * denom), 0.0)
    decay = jnp.where(live, 1.0 - 0.01 * 0.1, 1.0)
    eye = lax.broadcasted_iota(jnp.int32, (128, 128), 0) == lax.broadcasted_iota(jnp.int32, (128, 128), 1)
    for g in range(8):
        for i, value in enumerate((decay, rate)):
            column = jnp.sum(jnp.where(eye, value[g : g + 1, :], 0.0), axis=1, keepdims=True)
            coef[i, pl.ds(g * 128, 128), :] = jnp.broadcast_to(column, (128, 128))


def update(first, coef, scale, weights, new_weights, new_moment, new_scale):
    new_scale[...] = scale[...]
    for r in range(0, TALL, 16):
        rows = pl.ds(r, 16)
        decay, rate = coef[0, rows, :], coef[1, rows, :]
        for q in range(0, HALF, 128):
            columns = pl.ds(q, 128)
            value = first[rows, columns]
            new_moment[rows, columns] = value.astype(jnp.bfloat16)
            old = weights[rows, columns].astype(jnp.float32)
            new_weights[rows, columns] = (decay * old - rate * value).astype(jnp.bfloat16)


def over_pieces(value, axis):
    parts = lax.all_gather(value, axis)
    return parts.sum(axis=0)


def any_counts(token_grads, token_slot, slot_rows, counts, weights, moment, row_scale, row_steps):
    owners = lax.axis_size("vocab")
    slots_all = slot_rows.shape[1]
    cap = slots_all // owners
    half = token_grads.shape[1]
    rows_own = weights.shape[0]
    placing = token_slot[None, :] == jnp.arange(slots_all, dtype=jnp.int32)[:, None]
    slot_grads = jnp.dot(
        placing.astype(jnp.bfloat16), token_grads, preferred_element_type=jnp.float32
    ).astype(jnp.bfloat16)
    within = jnp.arange(cap, dtype=jnp.int32)
    live = within[None, :] < counts[0][:, None]
    named = jnp.where(live, slot_rows[0].reshape(owners, cap), -1)
    outgoing = slot_grads.reshape(owners, cap, half)
    received, received_rows = (
        lax.all_to_all(outgoing, "vocab", split_axis=0, concat_axis=0, tiled=True),
        lax.all_to_all(named, "vocab", split_axis=0, concat_axis=0, tiled=True),
    )
    flat = received.reshape(owners * cap, half)
    flat_rows = received_rows.reshape(owners * cap)
    table = flat_rows[None, :] == jnp.arange(rows_own, dtype=jnp.int32)[:, None]
    grad = jnp.dot(table.astype(jnp.bfloat16), flat, preferred_element_type=jnp.float32)
    hits = jnp.sum(table.astype(jnp.int32), axis=1)
    touched = hits > 0
    partial_sum = jnp.sum(grad * grad, axis=1)
    square = over_pieces(partial_sum, "width") / D
    step_count = (row_steps + 1).astype(jnp.float32)
    old_moment = moment.astype(jnp.float32)
    first = jnp.where(touched[:, None], 0.9 * old_moment + 0.1 * grad, old_moment)
    second = jnp.where(touched, 0.95 * row_scale + 0.05 * square, row_scale)
    fix_first = 1.0 - jnp.power(jnp.float32(0.9), step_count)
    fix_second = 1.0 - jnp.power(jnp.float32(0.95), step_count)
    denom = jnp.sqrt(second / fix_second) + 1e-08
    old = weights.astype(jnp.float32)
    stepped = old - 0.01 * (first / fix_first[:, None] / denom[:, None] + 0.1 * old)
    new_weights = jnp.where(touched[:, None], stepped, old).astype(jnp.bfloat16)
    return (new_weights, first.astype(jnp.bfloat16), second)


def shards(token_grads, token_slot, slot_rows, counts, weights, moment, row_scale, row_steps):
    vmem = pl.BlockSpec(memory_space=pltpu.VMEM)
    hbm = pl.BlockSpec(memory_space=pltpu.HBM)
    bf16, f32, i32 = jnp.bfloat16, jnp.float32, jnp.int32
    blocks = tuple(pltpu.VMEM((4, 4, 4, CAP, w), bf16) for w in WIDTH)
    first, coef, scale, weights_v, over = pl.pallas_call(
        exchange,
        name="exchange",
        out_shape=(
            pltpu.VMEM((ROWS, HALF), f32),
            pltpu.VMEM((2, ROWS, 128), f32),
            pltpu.VMEM((8, 128), f32),
            pltpu.VMEM((ROWS, HALF), bf16),
            jax.ShapeDtypeStruct((1, 128), i32),
        ),
        in_specs=[hbm] * 8,
        out_specs=(vmem,) * 5,
        scratch_shapes=[
            pltpu.VMEM((8, 128), i32),
            pltpu.VMEM((1, 1024), i32),
            pltpu.VMEM((1, 64), i32),
            pltpu.VMEM((8, 128), f32),
            pltpu.VMEM((8, 128), i32),
            pltpu.VMEM((ROWS, 128), f32),
            tuple(pltpu.VMEM((ROWS, w), bf16) for w in WIDTH),
            tuple(pltpu.VMEM((4, PLANE, w), bf16) for w in WIDTH),
            tuple(pltpu.VMEM((4, PLANE, w), bf16) for w in WIDTH),
            tuple(pltpu.VMEM((4, LINE, w), bf16) for w in WIDTH),
            tuple(pltpu.VMEM((4, LINE, w), bf16) for w in WIDTH),
            blocks,
            blocks,
            pltpu.VMEM((ROWS, ROWS), bf16),
            pltpu.VMEM((GROUPS, 4 * PLANE, ROWS), bf16),
            pltpu.VMEM((GROUPS, 4 * LINE, 4 * PLANE), bf16),
            pltpu.VMEM((GROUPS, ROWS, 4 * LINE), bf16),
            pltpu.VMEM((8, 8, 128), f32),
            pltpu.VMEM((3, 4, 1, 64), i32),
            pltpu.VMEM((3, 4, 4, 1, 64), i32),
            pltpu.VMEM((3, 4, 1, 128), i32),
            pltpu.VMEM((4, 4, 4, 1, 128), i32),
            pltpu.VMEM((4, 4, 4, 1, 128), i32),
            pltpu.VMEM((4, 4, 4, 1, 128), i32),
            pltpu.VMEM((4, 4, 4, 1, 128), i32),
            pltpu.VMEM((ROWS, 128), f32),
            pltpu.VMEM((8, 128), f32),
            pltpu.VMEM((8, 128), f32),
            pltpu.SemaphoreType.DMA((5,)),
            pltpu.SemaphoreType.DMA,
            pltpu.SemaphoreType.DMA((CHUNKS,)),
            pltpu.SemaphoreType.DMA((CHUNKS,)),
            pltpu.SemaphoreType.DMA((3, CHUNKS)),
            pltpu.SemaphoreType.DMA((3, CHUNKS)),
            pltpu.SemaphoreType.DMA((3,)),
            pltpu.SemaphoreType.DMA((3,)),
            pltpu.SemaphoreType.DMA((2,)),
            pltpu.SemaphoreType.DMA((4, 3)),
            pltpu.SemaphoreType.DMA((2, 3)),
        ],
        compiler_params=pltpu.CompilerParams(
            collective_id=0, has_side_effects=True, vmem_limit_bytes=46 * 1024 * 1024
        ),
        cost_estimate=pl.CostEstimate(flops=10**10, bytes_accessed=2 * 10**7, transcendentals=0),
    )(*(
        pltpu.with_memory_space_constraint(value, pltpu.HBM)
        for value in (
            token_grads, token_slot.reshape(8, 128), slot_rows, counts,
            row_scale.reshape(8, 128), row_steps.reshape(8, 128), weights, moment,
        )
    ))
    wide = pl.BlockSpec((TALL, HALF), lambda i: (i, 0))
    row = pl.BlockSpec((8, 128), lambda i: (0, 0))
    new_weights, new_moment, new_scale = pl.pallas_call(
        update,
        name="update",
        grid=(ROWS // TALL,),
        out_shape=(
            jax.ShapeDtypeStruct((ROWS, HALF), bf16),
            jax.ShapeDtypeStruct((ROWS, HALF), bf16),
            jax.ShapeDtypeStruct((8, 128), f32),
        ),
        in_specs=[wide, pl.BlockSpec((2, TALL, 128), lambda i: (0, i, 0)), row, wide],
        out_specs=(wide, wide, row),
        compiler_params=pltpu.CompilerParams(vmem_limit_bytes=10 * 1024 * 1024),
        cost_estimate=pl.CostEstimate(flops=2 * 10**7, bytes_accessed=3 * 10**7, transcendentals=0),
    )(first, coef, scale, weights_v)
    arguments = (token_grads, token_slot, slot_rows, counts, weights, moment, row_scale, row_steps)
    return lax.while_loop(
        lambda state: state[3] > 0,
        lambda state: any_counts(*arguments) + (jnp.int32(0),),
        (new_weights, new_moment, new_scale.reshape(ROWS), over[0, 0]),
    )[:3]


def solution(mesh):
    return jax.shard_map(
        shards,
        mesh=mesh,
        in_specs=(
            P("vocab", "width"),
            P("vocab"),
            P("vocab", None),
            P("vocab", None),
            P("vocab", "width"),
            P("vocab", "width"),
            P("vocab"),
            P("vocab"),
        ),
        out_specs=(P("vocab", "width"), P("vocab", "width"), P("vocab")),
        check_vma=False,
    )
```

```python
import functools
import jax
import jax.numpy as jnp
from jax import lax
from jax.experimental import pallas as pl
from jax.experimental.pallas import tpu as pltpu
from jax.sharding import PartitionSpec as P

D = 4608
HALF = 2304
ROWS = 1024
CAP = 16
PLANE = 128
LINE = 208
GROUPS = 3
WIDTHS = (256, 256, 256)
PER = len(WIDTHS)
CHUNKS = GROUPS * PER
WIDTH = WIDTHS * GROUPS
FIRST = tuple(sum(WIDTH[:c]) for c in range(CHUNKS))
TALL = 64
MESH = pl.DeviceIdType.MESH
ORDERS = ((0, 1, 2), (1, 2, 0), (2, 0, 1))


def to_row(column):
    eye = lax.broadcasted_iota(jnp.int32, (128, 128), 0) == lax.broadcasted_iota(jnp.int32, (128, 128), 1)
    parts = [
        jnp.sum(jnp.where(eye, column[g * 128 : g * 128 + 128, :], 0.0), axis=0, keepdims=True)
        for g in range(8)
    ]
    return jnp.concatenate(parts, axis=0)


def exchange(
    tg, ts_hbm, srows_hbm, cnts_hbm, rscale_hbm, rsteps_hbm, weights, moment,
    first, coef, scale, weights_v, over,
    ts, srows, cnts, rscale, rsteps, keep,
    tgv, s0, r1, s1, r2, s2, r3, onehot, place, pack, unpack, pbuf,
    ct1, ct2, flags, ms, m1, m2, m3, acc, sq_out, sq_in,
    small_sem, wide_sem, load_sem, moment_sem, send_sem, recv_sem, msend_sem, mrecv_sem, sq_sem,
    ct_sem, flag_sem,
):
    me = lax.axis_index("vocab")
    core = lax.axis_index("width")
    at = (me // 16, (me // 4) % 4, me % 4)
    stride = (16, 4, 1)

    def peer(dim, delta):
        there = (at[dim] + delta) % 4
        return there, (me + (there - at[dim]) * stride[dim], core)

    def load(c):
        return pltpu.make_async_copy(tg.at[:, pl.ds(FIRST[c], WIDTH[c])], tgv[c], load_sem.at[c])

    issue = [g * PER + k for k in range(PER) for g in range(GROUPS)]
    small = [
        pltpu.make_async_copy(src, dst, small_sem.at[i])
        for i, (src, dst) in enumerate(
            ((ts_hbm, ts), (srows_hbm, srows), (cnts_hbm, cnts), (rscale_hbm, rscale), (rsteps_hbm, rsteps))
        )
    ]
    for copy in small:
        copy.start()
    for c in issue:
        load(c).start()
    wide = pltpu.make_async_copy(weights, weights_v, wide_sem)

    def load_moment(c):
        return pltpu.make_async_copy(
            moment.at[:, pl.ds(FIRST[c], WIDTH[c])], tgv[c], moment_sem.at[c]
        )

    barrier = pltpu.get_barrier_semaphore()
    for dim in range(3):
        for delta in (1, 2, 3):
            pl.semaphore_signal(barrier, inc=1, device_id=peer(dim, delta)[1], device_id_type=MESH)
    partner = (me, 1 - core)
    pl.semaphore_signal(barrier, inc=1, device_id=partner, device_id_type=MESH)

    for copy in small:
        copy.wait()
    for rb in range(8):
        rows = lax.broadcasted_iota(jnp.int32, (128, 128), 0) + rb * 128
        for g in range(8):
            onehot[pl.ds(rb * 128, 128), pl.ds(g * 128, 128)] = (
                (rows == ts[g : g + 1, :]).astype(jnp.float32).astype(jnp.bfloat16)
            )

    def names_part(buf, phase, there):
        if phase == 0:
            return buf.at[there]
        return buf.at[:, there] if phase == 1 else buf.at[:, :, there]

    def post(src_of, dst, dim, ssem, rsem, own=True):
        for delta in (2, 1, 3):
            there, device = peer(dim, delta)
            pltpu.make_async_remote_copy(
                src_ref=src_of(there), dst_ref=dst,
                send_sem=ssem, recv_sem=rsem, device_id=device, device_id_type=MESH,
            ).start()
        if own:
            dst[...] = src_of(at[dim])[...]

    def post_names(phase):
        bufs = (ms, m1, m2, m3)
        post(
            lambda there: names_part(bufs[phase], phase, there),
            names_part(bufs[phase + 1], phase, at[phase]),
            phase, msend_sem.at[phase], mrecv_sem.at[phase],
        )

    def post_rows(phase, c):
        order = ORDERS[c // PER]
        dim = order[phase]
        src, dst = ((s0, r1), (s1, r2), (s2, r3))[phase]
        if phase < 2:
            target = dst[c].at[at[dim]]
        else:
            target = (dst[c].at[at[dim]], dst[c].at[:, at[dim]], dst[c].at[:, :, at[dim]])[dim]
        post(lambda there: src[c].at[there], target, dim, send_sem.at[phase, c], recv_sem.at[phase, c])

    def take(blocks, sem):
        whole = blocks.at[pl.ds(0, 3)]
        pltpu.make_async_copy(whole, whole, sem).wait()

    staged = (s0, s1, s2)

    def take_rows(phase, c):
        take(staged[phase][c], recv_sem.at[phase, c])

    def coordinate(owner, dim):
        return (owner // stride[dim]) % 4

    lane_g = lax.broadcasted_iota(jnp.int32, (64, 128), 1) // CAP
    own_g = lax.broadcasted_iota(jnp.int32, (64, 128), 0) % 8
    spread = (lane_g == own_g).astype(jnp.float32)
    owner8 = lax.broadcasted_iota(jnp.int32, (8, 64), 1) // 8
    by_block = jnp.where(
        owner8 == lax.broadcasted_iota(jnp.int32, (8, 64), 0), cnts[...].astype(jnp.float32), 0.0
    )
    count = jnp.dot(by_block, spread, preferred_element_type=jnp.float32)
    lanes = lax.broadcasted_iota(jnp.int32, (8, 128), 1)
    names = jnp.concatenate([srows[:, g * 128 : g * 128 + 128] for g in range(8)], axis=0)
    names = jnp.where((lanes % CAP).astype(jnp.float32) < count, names + 1, 0)
    for j in range(8):
        turned = pltpu.roll(names, ((me % 8) - j + 8) % 8 * CAP, 1)
        turned = jnp.where(lanes // CAP == me % 8, turned, 0)
        for g in range(8):
            o = 8 * g + j
            ms[o // 16, (o // 4) % 4, o % 4] = turned[g : g + 1, :]


    cnt8 = jnp.broadcast_to(cnts[...].astype(jnp.float32), (8, 64))
    o_from = lax.broadcasted_iota(jnp.int32, (64, 64), 0)
    o_to = lax.broadcasted_iota(jnp.int32, (64, 64), 1)
    o_slot = lax.broadcasted_iota(jnp.int32, (8, 128), 0) * 8 + lanes // CAP
    excess = jnp.zeros((8, 64), jnp.float32)
    for g, (a, b, c) in enumerate(ORDERS):
        same = coordinate(o_from, a) == coordinate(o_to, a)
        ahead = same & (
            coordinate(o_from, b) * 4 + coordinate(o_from, c)
            < coordinate(o_to, b) * 4 + coordinate(o_to, c)
        )
        before = jnp.dot(cnt8, ahead.astype(jnp.float32), preferred_element_type=jnp.float32)
        total = jnp.dot(cnt8, same.astype(jnp.float32), preferred_element_type=jnp.float32)
        excess = jnp.maximum(excess, total - PLANE)
        before = jnp.where(owner8 == lax.broadcasted_iota(jnp.int32, (8, 64), 0), before, 0.0)
        before = jnp.dot(before, spread, preferred_element_type=jnp.float32)
        place_at = (coordinate(o_slot, a) * PLANE + lanes % CAP).astype(jnp.float32) + before
        high = jnp.floor(place_at * (1.0 / 32.0))
        low = place_at - 32.0 * high
        for blk in range(8):
            pbuf[blk, pl.ds(2 * g, 1), :] = high[blk : blk + 1, :]
            pbuf[blk, pl.ds(2 * g + 1, 1), :] = low[blk : blk + 1, :]
    for blk in range(8):
        pbuf[blk, pl.ds(6, 2), :] = jnp.zeros((2, 128), jnp.float32)
    token_at = jnp.zeros((8, ROWS), jnp.float32)
    for blk in range(8):
        token_at = token_at + jnp.dot(
            pbuf[blk].astype(jnp.bfloat16), onehot[pl.ds(blk * 128, 128), :],
            preferred_element_type=jnp.float32,
        )
    for g in range(GROUPS):
        where_to = 32.0 * token_at[2 * g : 2 * g + 1, :] + token_at[2 * g + 1 : 2 * g + 2, :]
        for rb in range(0, 4 * PLANE, 128):
            rows = (lax.broadcasted_iota(jnp.int32, (128, ROWS), 0) + rb).astype(jnp.float32)
            place[g, pl.ds(rb, 128), :] = (rows == where_to).astype(jnp.float32).astype(jnp.bfloat16)

    pl.semaphore_wait(barrier, 10)
    for dim in range(3):
        post(lambda there: cnts, ct1.at[dim, at[dim]], dim, ct_sem.at[0, dim], ct_sem.at[1, dim])
    post_names(0)

    for c in issue:
        load(c).wait()
        s0[c][...] = (
            jnp.dot(place[c // PER], tgv[c][...], preferred_element_type=jnp.float32)
            .astype(jnp.bfloat16)
            .reshape(4, PLANE, WIDTH[c])
        )
        post_rows(0, c)

    b_of = lax.broadcasted_iota(jnp.int32, (8, 64), 0)
    o_line = lax.broadcasted_iota(jnp.int32, (8, 64), 1)
    ones = jnp.ones((64, 128), jnp.float32)
    excess = jnp.max(jnp.max(excess, axis=1, keepdims=True), axis=0, keepdims=True)
    idx = lanes.astype(jnp.float32)
    line_at = (lax.broadcasted_iota(jnp.int32, (8, 128), 0) * LINE).astype(jnp.float32)
    for dim in range(3):
        take(ct1.at[dim], ct_sem.at[1, dim])
    for g, (a, b, c) in enumerate(ORDERS):
        post(
            lambda there: ct1.at[a], ct2.at[g, at[b]], b, ct_sem.at[2, g], ct_sem.at[3, g]
        )
        in_plane = coordinate(o_line, a) == at[a]
        b_owner = coordinate(o_line, b)
        base = jnp.zeros((8, 128), jnp.float32)
        for source in range(4):
            row = jnp.broadcast_to(ct1[a, source].astype(jnp.float32), (8, 64))
            offset = jnp.dot(
                jnp.where(in_plane & (b_owner < b_of), row, 0.0), ones, preferred_element_type=jnp.float32
            )
            length = jnp.dot(
                jnp.where(in_plane & (b_owner == b_of), row, 0.0), ones, preferred_element_type=jnp.float32
            )
            inside = (idx >= offset) & (idx < offset + length)
            goes = jnp.sum(
                jnp.where(inside, line_at + base + idx - offset + 1.0, 0.0), axis=0, keepdims=True
            )
            for rb in range(0, 4 * LINE, 208):
                rows = (lax.broadcasted_iota(jnp.int32, (208, 128), 0) + (rb + 1)).astype(jnp.float32)
                pack[g, pl.ds(rb, 208), pl.ds(source * 128, 128)] = (
                    (rows == goes).astype(jnp.float32).astype(jnp.bfloat16)
                )
            base = base + length
        most = jnp.max(base - LINE, axis=0, keepdims=True)
        excess = jnp.maximum(excess, most)
    flags[0, at[0]] = jnp.where(excess > 0.0, 1, 0)

    def post_flag(dim):
        post(
            lambda there: flags.at[dim, at[dim]], flags.at[dim, at[dim]], dim,
            flag_sem.at[0, dim], flag_sem.at[1, dim], own=False,
        )

    take(m1, mrecv_sem.at[0])
    post_names(1)
    for n, c in enumerate(issue):
        take_rows(0, c)
        s1[c][...] = (
            jnp.dot(pack[c // PER], r1[c][...].reshape(4 * PLANE, WIDTH[c]), preferred_element_type=jnp.float32)
            .astype(jnp.bfloat16)
            .reshape(4, LINE, WIDTH[c])
        )
        post_rows(1, c)
        load_moment(c).start()
        if n == 0:
            post_flag(0)
        if n == 2:
            take(m1, mrecv_sem.at[1])
            post_names(2)
            take(flags.at[0], flag_sem.at[1, 0])
            flags[1, at[1]] = jnp.max(flags[0], axis=0)
        if n == 3:
            post_flag(1)
        if n == 5:
            take(flags.at[1], flag_sem.at[1, 1])
            flags[2, at[2]] = jnp.max(flags[1], axis=0)
        if n == 6:
            post_flag(2)
    wide.start()

    unit = lax.broadcasted_iota(jnp.int32, (64, 64), 0)
    slot_unit = (
        lax.broadcasted_iota(jnp.int32, (ROWS, 64), 0) // CAP == lax.broadcasted_iota(jnp.int32, (ROWS, 64), 1)
    ).astype(jnp.float32)
    slot = lax.broadcasted_iota(jnp.int32, (ROWS, 128), 0)
    for g, (a, b, c) in enumerate(ORDERS):
        take(ct2.at[g], ct_sem.at[3, g])
        c_unit = unit // 16
        a_unit, b_unit = ((unit // 4) % 4, unit % 4) if a < b else (unit % 4, (unit // 4) % 4)
        in_line = (coordinate(o_to, a) == at[a]) & (coordinate(o_to, b) == at[b])
        c_owner = coordinate(o_to, c)
        begin = jnp.zeros((64, 64), jnp.float32)
        size = jnp.zeros((64, 64), jnp.float32)
        for sb in range(4):
            for sa in range(4):
                row = jnp.broadcast_to(ct2[g, sb, sa].astype(jnp.float32), (64, 64))
                row = jnp.where(in_line & (b_unit == sb), row, 0.0)
                begin = begin + jnp.where(
                    (a_unit > sa) | ((a_unit == sa) & (c_owner < c_unit)), row, 0.0
                )
                size = size + jnp.where((a_unit == sa) & (c_owner == c_unit), row, 0.0)
        begin = jnp.dot(begin, ones, preferred_element_type=jnp.float32)
        size = jnp.dot(size, ones, preferred_element_type=jnp.float32)
        begin = jnp.dot(slot_unit, begin, preferred_element_type=jnp.float32)
        size = jnp.dot(slot_unit, size, preferred_element_type=jnp.float32)
        within = (slot % CAP).astype(jnp.float32)
        sb_slot = (slot // CAP) % 4 if a < b else (slot // (CAP * 4)) % 4
        comes = jnp.where(
            within < size, (sb_slot * LINE).astype(jnp.float32) + begin + within, -1.0
        )
        for q in range(0, 4 * LINE, 128):
            span = min(128, 4 * LINE - q)
            columns = (lax.broadcasted_iota(jnp.int32, (ROWS, span), 1) + q).astype(jnp.float32)
            unpack[g, :, pl.ds(q, span)] = (
                (columns == comes[:, :span]).astype(jnp.float32).astype(jnp.bfloat16)
            )

    for c in issue:
        take_rows(1, c)
        s2[c][...] = (
            jnp.dot(unpack[c // PER], r2[c][...].reshape(4 * LINE, WIDTH[c]), preferred_element_type=jnp.float32)
            .astype(jnp.bfloat16)
            .reshape(4, 4, 4, CAP, WIDTH[c])
        )
        post_rows(2, c)

    take(m1, mrecv_sem.at[2])
    named = m3[...].reshape(8, 8, 128).sum(axis=1)
    touched_parts = []
    for rb in range(8):
        rows = lax.broadcasted_iota(jnp.int32, (128, 128), 0) + (rb * 128 + 1)
        any_hit = jnp.zeros((128, 128), jnp.float32)
        for g in range(8):
            hit = (rows == named[g : g + 1, :]).astype(jnp.float32)
            onehot[pl.ds(rb * 128, 128), pl.ds(g * 128, 128)] = hit.astype(jnp.bfloat16)
            any_hit = jnp.maximum(any_hit, hit)
        hit_column = jnp.max(any_hit, axis=1, keepdims=True)
        touched_parts.append(hit_column)
        keep[pl.ds(rb * 128, 128), :] = jnp.broadcast_to(1.0 - 0.1 * hit_column, (128, 128))
    touched = to_row(jnp.concatenate(touched_parts, axis=0))
    steps = (rsteps[...] + 1).astype(jnp.float32)
    fix_first = 1.0 - jnp.exp(steps * jnp.log(jnp.float32(0.9)))
    fix_second = 1.0 - jnp.exp(steps * jnp.log(jnp.float32(0.95)))

    for n, c in enumerate(issue):
        take_rows(2, c)
        load_moment(c).wait()
        received = r3[c][...].reshape(ROWS, WIDTH[c])
        for rb in range(8):
            rows = pl.ds(rb * 128, 128)
            part = jnp.dot(onehot[rows, :], received, preferred_element_type=jnp.float32)
            folded = None
            for q in range(0, WIDTH[c], 128):
                columns = pl.ds(FIRST[c] + q, 128)
                piece = part[:, q : q + 128]
                first[rows, columns] = (
                    keep[rows, :] * tgv[c][rows, pl.ds(q, 128)].astype(jnp.float32) + 0.1 * piece
                )
                folded = piece * piece if folded is None else folded + piece * piece
            if n == 0:
                acc[rows, :] = folded
            else:
                acc[rows, :] += folded

    mine = to_row(jnp.sum(acc[...], axis=1, keepdims=True))
    sq_out[...] = mine
    swap = pltpu.make_async_remote_copy(
        src_ref=sq_out, dst_ref=sq_in, send_sem=sq_sem.at[0], recv_sem=sq_sem.at[1],
        device_id=partner, device_id_type=MESH,
    )
    swap.start()

    for phase in range(3):
        for c in range(CHUNKS):
            take(staged[phase][c], send_sem.at[phase, c])
        take(m1, msend_sem.at[phase])
        take(ct1.at[0], ct_sem.at[0, phase])
        take(ct2.at[0], ct_sem.at[2, phase])
        take(flags.at[0], flag_sem.at[0, phase])
    take(flags.at[2], flag_sem.at[1, 2])
    over[...] = jnp.max(flags[2], axis=0)
    wide.wait()
    swap.wait()

    square = (mine + sq_in[...]) / D
    live = touched > 0.0
    second = jnp.where(live, 0.95 * rscale[...] + 0.05 * square, rscale[...])
    scale[...] = second
    denom = jnp.sqrt(second / fix_second) + 1e-08
    rate = jnp.where(live, 0.01 / (fix_first * denom), 0.0)
    decay = jnp.where(live, 1.0 - 0.01 * 0.1, 1.0)
    eye = lax.broadcasted_iota(jnp.int32, (128, 128), 0) == lax.broadcasted_iota(jnp.int32, (128, 128), 1)
    for g in range(8):
        for i, value in enumerate((decay, rate)):
            column = jnp.sum(jnp.where(eye, value[g : g + 1, :], 0.0), axis=1, keepdims=True)
            coef[i, pl.ds(g * 128, 128), :] = jnp.broadcast_to(column, (128, 128))


def update(first, coef, scale, weights, new_weights, new_moment, new_scale, made_w, made_m, sem, scale_sem):
    out_scale = pltpu.make_async_copy(scale, new_scale, scale_sem)
    out_scale.start()
    copies = []
    for n in range(ROWS // TALL):
        block = pl.ds(n * TALL, TALL)

        def some(r, carry, n=n):
            rows = pl.ds(pl.multiple_of(n * TALL + r * 16, 16), 16)
            decay, rate = coef[0, rows, :], coef[1, rows, :]
            for q in range(0, HALF, 128):
                columns = pl.ds(q, 128)
                value = first[rows, columns]
                made_m[rows, columns] = value.astype(jnp.bfloat16)
                old = weights[rows, columns].astype(jnp.float32)
                made_w[rows, columns] = (decay * old - rate * value).astype(jnp.bfloat16)
            return carry

        lax.fori_loop(0, TALL // 16, some, 0)
        for i, (src, dst) in enumerate(((made_m, new_moment), (made_w, new_weights))):
            copy = pltpu.make_async_copy(src.at[block, :], dst.at[block, :], sem.at[i, n])
            copy.start()
            copies.append(copy)
    for copy in copies:
        copy.wait()
    out_scale.wait()


def over_pieces(value, axis):
    parts = lax.all_gather(value, axis)
    return parts.sum(axis=0)


def any_counts(token_grads, token_slot, slot_rows, counts, weights, moment, row_scale, row_steps):
    owners = lax.axis_size("vocab")
    slots_all = slot_rows.shape[1]
    cap = slots_all // owners
    half = token_grads.shape[1]
    rows_own = weights.shape[0]
    placing = token_slot[None, :] == jnp.arange(slots_all, dtype=jnp.int32)[:, None]
    slot_grads = jnp.dot(
        placing.astype(jnp.bfloat16), token_grads, preferred_element_type=jnp.float32
    ).astype(jnp.bfloat16)
    within = jnp.arange(cap, dtype=jnp.int32)
    live = within[None, :] < counts[0][:, None]
    named = jnp.where(live, slot_rows[0].reshape(owners, cap), -1)
    outgoing = slot_grads.reshape(owners, cap, half)
    received, received_rows = (
        lax.all_to_all(outgoing, "vocab", split_axis=0, concat_axis=0, tiled=True),
        lax.all_to_all(named, "vocab", split_axis=0, concat_axis=0, tiled=True),
    )
    flat = received.reshape(owners * cap, half)
    flat_rows = received_rows.reshape(owners * cap)
    table = flat_rows[None, :] == jnp.arange(rows_own, dtype=jnp.int32)[:, None]
    grad = jnp.dot(table.astype(jnp.bfloat16), flat, preferred_element_type=jnp.float32)
    hits = jnp.sum(table.astype(jnp.int32), axis=1)
    touched = hits > 0
    partial_sum = jnp.sum(grad * grad, axis=1)
    square = over_pieces(partial_sum, "width") / D
    step_count = (row_steps + 1).astype(jnp.float32)
    old_moment = moment.astype(jnp.float32)
    first = jnp.where(touched[:, None], 0.9 * old_moment + 0.1 * grad, old_moment)
    second = jnp.where(touched, 0.95 * row_scale + 0.05 * square, row_scale)
    fix_first = 1.0 - jnp.power(jnp.float32(0.9), step_count)
    fix_second = 1.0 - jnp.power(jnp.float32(0.95), step_count)
    denom = jnp.sqrt(second / fix_second) + 1e-08
    old = weights.astype(jnp.float32)
    stepped = old - 0.01 * (first / fix_first[:, None] / denom[:, None] + 0.1 * old)
    new_weights = jnp.where(touched[:, None], stepped, old).astype(jnp.bfloat16)
    return (new_weights, first.astype(jnp.bfloat16), second)


def shards(token_grads, token_slot, slot_rows, counts, weights, moment, row_scale, row_steps):
    vmem = pl.BlockSpec(memory_space=pltpu.VMEM)
    hbm = pl.BlockSpec(memory_space=pltpu.HBM)
    bf16, f32, i32 = jnp.bfloat16, jnp.float32, jnp.int32
    blocks = tuple(pltpu.VMEM((4, 4, 4, CAP, w), bf16) for w in WIDTH)
    first, coef, scale, weights_v, over = pl.pallas_call(
        exchange,
        name="exchange",
        out_shape=(
            pltpu.VMEM((ROWS, HALF), f32),
            pltpu.VMEM((2, ROWS, 128), f32),
            pltpu.VMEM((8, 128), f32),
            pltpu.VMEM((ROWS, HALF), bf16),
            jax.ShapeDtypeStruct((1, 128), i32),
        ),
        in_specs=[hbm] * 8,
        out_specs=(vmem,) * 5,
        scratch_shapes=[
            pltpu.VMEM((8, 128), i32),
            pltpu.VMEM((1, 1024), i32),
            pltpu.VMEM((1, 64), i32),
            pltpu.VMEM((8, 128), f32),
            pltpu.VMEM((8, 128), i32),
            pltpu.VMEM((ROWS, 128), f32),
            tuple(pltpu.VMEM((ROWS, w), bf16) for w in WIDTH),
            tuple(pltpu.VMEM((4, PLANE, w), bf16) for w in WIDTH),
            tuple(pltpu.VMEM((4, PLANE, w), bf16) for w in WIDTH),
            tuple(pltpu.VMEM((4, LINE, w), bf16) for w in WIDTH),
            tuple(pltpu.VMEM((4, LINE, w), bf16) for w in WIDTH),
            blocks,
            blocks,
            pltpu.VMEM((ROWS, ROWS), bf16),
            pltpu.VMEM((GROUPS, 4 * PLANE, ROWS), bf16),
            pltpu.VMEM((GROUPS, 4 * LINE, 4 * PLANE), bf16),
            pltpu.VMEM((GROUPS, ROWS, 4 * LINE), bf16),
            pltpu.VMEM((8, 8, 128), f32),
            pltpu.VMEM((3, 4, 1, 64), i32),
            pltpu.VMEM((3, 4, 4, 1, 64), i32),
            pltpu.VMEM((3, 4, 1, 128), i32),
            pltpu.VMEM((4, 4, 4, 1, 128), i32),
            pltpu.VMEM((4, 4, 4, 1, 128), i32),
            pltpu.VMEM((4, 4, 4, 1, 128), i32),
            pltpu.VMEM((4, 4, 4, 1, 128), i32),
            pltpu.VMEM((ROWS, 128), f32),
            pltpu.VMEM((8, 128), f32),
            pltpu.VMEM((8, 128), f32),
            pltpu.SemaphoreType.DMA((5,)),
            pltpu.SemaphoreType.DMA,
            pltpu.SemaphoreType.DMA((CHUNKS,)),
            pltpu.SemaphoreType.DMA((CHUNKS,)),
            pltpu.SemaphoreType.DMA((3, CHUNKS)),
            pltpu.SemaphoreType.DMA((3, CHUNKS)),
            pltpu.SemaphoreType.DMA((3,)),
            pltpu.SemaphoreType.DMA((3,)),
            pltpu.SemaphoreType.DMA((2,)),
            pltpu.SemaphoreType.DMA((4, 3)),
            pltpu.SemaphoreType.DMA((2, 3)),
        ],
        compiler_params=pltpu.CompilerParams(
            collective_id=0, has_side_effects=True, vmem_limit_bytes=46 * 1024 * 1024
        ),
        cost_estimate=pl.CostEstimate(flops=10**10, bytes_accessed=2 * 10**7, transcendentals=0),
    )(*(
        pltpu.with_memory_space_constraint(value, pltpu.HBM)
        for value in (
            token_grads, token_slot.reshape(8, 128), slot_rows, counts,
            row_scale.reshape(8, 128), row_steps.reshape(8, 128), weights, moment,
        )
    ))
    new_weights, new_moment, new_scale = pl.pallas_call(
        update,
        name="update",
        out_shape=(
            jax.ShapeDtypeStruct((ROWS, HALF), bf16),
            jax.ShapeDtypeStruct((ROWS, HALF), bf16),
            jax.ShapeDtypeStruct((8, 128), f32),
        ),
        in_specs=[vmem] * 4,
        out_specs=(hbm,) * 3,
        scratch_shapes=[
            pltpu.VMEM((ROWS, HALF), bf16),
            pltpu.VMEM((ROWS, HALF), bf16),
            pltpu.SemaphoreType.DMA((2, ROWS // TALL)),
            pltpu.SemaphoreType.DMA,
        ],
        compiler_params=pltpu.CompilerParams(vmem_limit_bytes=12 * 1024 * 1024),
        cost_estimate=pl.CostEstimate(flops=2 * 10**7, bytes_accessed=3 * 10**7, transcendentals=0),
    )(first, coef, scale, weights_v)
    arguments = (token_grads, token_slot, slot_rows, counts, weights, moment, row_scale, row_steps)
    return lax.while_loop(
        lambda state: state[3] > 0,
        lambda state: any_counts(*arguments) + (jnp.int32(0),),
        (new_weights, new_moment, new_scale.reshape(ROWS), over[0, 0]),
    )[:3]


def solution(mesh):
    return jax.shard_map(
        shards,
        mesh=mesh,
        in_specs=(
            P("vocab", "width"),
            P("vocab"),
            P("vocab", None),
            P("vocab", None),
            P("vocab", "width"),
            P("vocab", "width"),
            P("vocab"),
            P("vocab"),
        ),
        out_specs=(P("vocab", "width"), P("vocab", "width"), P("vocab")),
        check_vma=False,
    )
```

```python
import functools
import jax
import jax.numpy as jnp
from jax import lax
from jax.experimental import pallas as pl
from jax.experimental.pallas import tpu as pltpu
from jax.sharding import PartitionSpec as P

D = 4608
HALF = 2304
ROWS = 1024
CAP = 16
PLANE = 128
LINE = 208
GROUPS = 3
WIDTHS = (256, 256, 256)
PER = len(WIDTHS)
CHUNKS = GROUPS * PER
WIDTH = WIDTHS * GROUPS
FIRST = tuple(sum(WIDTH[:c]) for c in range(CHUNKS))
TALL = 64
MESH = pl.DeviceIdType.MESH
ORDERS = ((0, 1, 2), (1, 2, 0), (2, 0, 1))


def to_row(column):
    eye = lax.broadcasted_iota(jnp.int32, (128, 128), 0) == lax.broadcasted_iota(jnp.int32, (128, 128), 1)
    parts = [
        jnp.sum(jnp.where(eye, column[g * 128 : g * 128 + 128, :], 0.0), axis=0, keepdims=True)
        for g in range(8)
    ]
    return jnp.concatenate(parts, axis=0)


def exchange(
    tg, ts_hbm, srows_hbm, cnts_hbm, rscale_hbm, rsteps_hbm, weights, moment,
    first, coef, scale, weights_v, over,
    ts, srows, cnts, rscale, rsteps, keep,
    tgv, s0, r1, s1, r2, s2, r3, onehot, place, pack, unpack, pbuf,
    ct1, ct2, flags, ms, m1, m2, m3, acc, sq_out, sq_in,
    small_sem, wide_sem, load_sem, moment_sem, send_sem, recv_sem, msend_sem, mrecv_sem, sq_sem,
    ct_sem, flag_sem,
):
    me = lax.axis_index("vocab")
    core = lax.axis_index("width")
    at = (me // 16, (me // 4) % 4, me % 4)
    stride = (16, 4, 1)

    def peer(dim, delta):
        there = (at[dim] + delta) % 4
        return there, (me + (there - at[dim]) * stride[dim], core)

    def load(c):
        return pltpu.make_async_copy(tg.at[:, pl.ds(FIRST[c], WIDTH[c])], tgv[c], load_sem.at[c])

    issue = [g * PER + k for k in range(PER) for g in range(GROUPS)]
    small = [
        pltpu.make_async_copy(src, dst, small_sem.at[i])
        for i, (src, dst) in enumerate(
            ((ts_hbm, ts), (srows_hbm, srows), (cnts_hbm, cnts), (rscale_hbm, rscale), (rsteps_hbm, rsteps))
        )
    ]
    for copy in small:
        copy.start()
    for c in issue:
        load(c).start()
    wide = pltpu.make_async_copy(weights, weights_v, wide_sem)

    def load_moment(c):
        return pltpu.make_async_copy(
            moment.at[:, pl.ds(FIRST[c], WIDTH[c])], tgv[c], moment_sem.at[c]
        )

    barrier = pltpu.get_barrier_semaphore()
    for dim in range(3):
        for delta in (1, 2, 3):
            pl.semaphore_signal(barrier, inc=1, device_id=peer(dim, delta)[1], device_id_type=MESH)
    partner = (me, 1 - core)
    pl.semaphore_signal(barrier, inc=1, device_id=partner, device_id_type=MESH)

    for copy in small:
        copy.wait()
    for rb in range(8):
        rows = lax.broadcasted_iota(jnp.int32, (128, 128), 0) + rb * 128
        for g in range(8):
            onehot[pl.ds(rb * 128, 128), pl.ds(g * 128, 128)] = (
                (rows == ts[g : g + 1, :]).astype(jnp.float32).astype(jnp.bfloat16)
            )

    def names_part(buf, phase, there):
        if phase == 0:
            return buf.at[there]
        return buf.at[:, there] if phase == 1 else buf.at[:, :, there]

    def post(src_of, dst, dim, ssem, rsem, own=True):
        for delta in (1, 3, 2):
            there, device = peer(dim, delta)
            pltpu.make_async_remote_copy(
                src_ref=src_of(there), dst_ref=dst,
                send_sem=ssem, recv_sem=rsem, device_id=device, device_id_type=MESH,
            ).start()
        if own:
            dst[...] = src_of(at[dim])[...]

    def post_names(phase):
        bufs = (ms, m1, m2, m3)
        post(
            lambda there: names_part(bufs[phase], phase, there),
            names_part(bufs[phase + 1], phase, at[phase]),
            phase, msend_sem.at[phase], mrecv_sem.at[phase],
        )

    def post_rows(phase, c):
        order = ORDERS[c // PER]
        dim = order[phase]
        src, dst = ((s0, r1), (s1, r2), (s2, r3))[phase]
        if phase < 2:
            target = dst[c].at[at[dim]]
        else:
            target = (dst[c].at[at[dim]], dst[c].at[:, at[dim]], dst[c].at[:, :, at[dim]])[dim]
        post(lambda there: src[c].at[there], target, dim, send_sem.at[phase, c], recv_sem.at[phase, c])

    def take(blocks, sem):
        whole = blocks.at[pl.ds(0, 3)]
        pltpu.make_async_copy(whole, whole, sem).wait()

    staged = (s0, s1, s2)

    def take_rows(phase, c):
        take(staged[phase][c], recv_sem.at[phase, c])

    def coordinate(owner, dim):
        return (owner // stride[dim]) % 4

    lane_g = lax.broadcasted_iota(jnp.int32, (64, 128), 1) // CAP
    own_g = lax.broadcasted_iota(jnp.int32, (64, 128), 0) % 8
    spread = (lane_g == own_g).astype(jnp.float32)
    owner8 = lax.broadcasted_iota(jnp.int32, (8, 64), 1) // 8
    by_block = jnp.where(
        owner8 == lax.broadcasted_iota(jnp.int32, (8, 64), 0), cnts[...].astype(jnp.float32), 0.0
    )
    count = jnp.dot(by_block, spread, preferred_element_type=jnp.float32)
    lanes = lax.broadcasted_iota(jnp.int32, (8, 128), 1)
    names = jnp.concatenate([srows[:, g * 128 : g * 128 + 128] for g in range(8)], axis=0)
    names = jnp.where((lanes % CAP).astype(jnp.float32) < count, names + 1, 0)
    for j in range(8):
        turned = pltpu.roll(names, ((me % 8) - j + 8) % 8 * CAP, 1)
        turned = jnp.where(lanes // CAP == me % 8, turned, 0)
        for g in range(8):
            o = 8 * g + j
            ms[o // 16, (o // 4) % 4, o % 4] = turned[g : g + 1, :]


    cnt8 = jnp.broadcast_to(cnts[...].astype(jnp.float32), (8, 64))
    o_from = lax.broadcasted_iota(jnp.int32, (64, 64), 0)
    o_to = lax.broadcasted_iota(jnp.int32, (64, 64), 1)
    o_slot = lax.broadcasted_iota(jnp.int32, (8, 128), 0) * 8 + lanes // CAP
    excess = jnp.zeros((8, 64), jnp.float32)
    for g, (a, b, c) in enumerate(ORDERS):
        same = coordinate(o_from, a) == coordinate(o_to, a)
        ahead = same & (
            coordinate(o_from, b) * 4 + coordinate(o_from, c)
            < coordinate(o_to, b) * 4 + coordinate(o_to, c)
        )
        before = jnp.dot(cnt8, ahead.astype(jnp.float32), preferred_element_type=jnp.float32)
        total = jnp.dot(cnt8, same.astype(jnp.float32), preferred_element_type=jnp.float32)
        excess = jnp.maximum(excess, total - PLANE)
        before = jnp.where(owner8 == lax.broadcasted_iota(jnp.int32, (8, 64), 0), before, 0.0)
        before = jnp.dot(before, spread, preferred_element_type=jnp.float32)
        place_at = (coordinate(o_slot, a) * PLANE + lanes % CAP).astype(jnp.float32) + before
        high = jnp.floor(place_at * (1.0 / 32.0))
        low = place_at - 32.0 * high
        for blk in range(8):
            pbuf[blk, pl.ds(2 * g, 1), :] = high[blk : blk + 1, :]
            pbuf[blk, pl.ds(2 * g + 1, 1), :] = low[blk : blk + 1, :]
    for blk in range(8):
        pbuf[blk, pl.ds(6, 2), :] = jnp.zeros((2, 128), jnp.float32)
    token_at = jnp.zeros((8, ROWS), jnp.float32)
    for blk in range(8):
        token_at = token_at + jnp.dot(
            pbuf[blk].astype(jnp.bfloat16), onehot[pl.ds(blk * 128, 128), :],
            preferred_element_type=jnp.float32,
        )
    for g in range(GROUPS):
        where_to = 32.0 * token_at[2 * g : 2 * g + 1, :] + token_at[2 * g + 1 : 2 * g + 2, :]
        for rb in range(0, 4 * PLANE, 128):
            rows = (lax.broadcasted_iota(jnp.int32, (128, ROWS), 0) + rb).astype(jnp.float32)
            place[g, pl.ds(rb, 128), :] = (rows == where_to).astype(jnp.float32).astype(jnp.bfloat16)

    pl.semaphore_wait(barrier, 10)
    for dim in range(3):
        post(lambda there: cnts, ct1.at[dim, at[dim]], dim, ct_sem.at[0, dim], ct_sem.at[1, dim])
    post_names(0)

    for c in issue:
        load(c).wait()
        s0[c][...] = (
            jnp.dot(place[c // PER], tgv[c][...], preferred_element_type=jnp.float32)
            .astype(jnp.bfloat16)
            .reshape(4, PLANE, WIDTH[c])
        )
        post_rows(0, c)

    b_of = lax.broadcasted_iota(jnp.int32, (8, 64), 0)
    o_line = lax.broadcasted_iota(jnp.int32, (8, 64), 1)
    ones = jnp.ones((64, 128), jnp.float32)
    excess = jnp.max(jnp.max(excess, axis=1, keepdims=True), axis=0, keepdims=True)
    idx = lanes.astype(jnp.float32)
    line_at = (lax.broadcasted_iota(jnp.int32, (8, 128), 0) * LINE).astype(jnp.float32)
    for dim in range(3):
        take(ct1.at[dim], ct_sem.at[1, dim])
    for g, (a, b, c) in enumerate(ORDERS):
        post(
            lambda there: ct1.at[a], ct2.at[g, at[b]], b, ct_sem.at[2, g], ct_sem.at[3, g]
        )
        in_plane = coordinate(o_line, a) == at[a]
        b_owner = coordinate(o_line, b)
        base = jnp.zeros((8, 128), jnp.float32)
        for source in range(4):
            row = jnp.broadcast_to(ct1[a, source].astype(jnp.float32), (8, 64))
            offset = jnp.dot(
                jnp.where(in_plane & (b_owner < b_of), row, 0.0), ones, preferred_element_type=jnp.float32
            )
            length = jnp.dot(
                jnp.where(in_plane & (b_owner == b_of), row, 0.0), ones, preferred_element_type=jnp.float32
            )
            inside = (idx >= offset) & (idx < offset + length)
            goes = jnp.sum(
                jnp.where(inside, line_at + base + idx - offset + 1.0, 0.0), axis=0, keepdims=True
            )
            for rb in range(0, 4 * LINE, 208):
                rows = (lax.broadcasted_iota(jnp.int32, (208, 128), 0) + (rb + 1)).astype(jnp.float32)
                pack[g, pl.ds(rb, 208), pl.ds(source * 128, 128)] = (
                    (rows == goes).astype(jnp.float32).astype(jnp.bfloat16)
                )
            base = base + length
        most = jnp.max(base - LINE, axis=0, keepdims=True)
        excess = jnp.maximum(excess, most)
    flags[0, at[0]] = jnp.where(excess > 0.0, 1, 0)

    def post_flag(dim):
        post(
            lambda there: flags.at[dim, at[dim]], flags.at[dim, at[dim]], dim,
            flag_sem.at[0, dim], flag_sem.at[1, dim], own=False,
        )

    take(m1, mrecv_sem.at[0])
    post_names(1)
    for n, c in enumerate(issue):
        take_rows(0, c)
        s1[c][...] = (
            jnp.dot(pack[c // PER], r1[c][...].reshape(4 * PLANE, WIDTH[c]), preferred_element_type=jnp.float32)
            .astype(jnp.bfloat16)
            .reshape(4, LINE, WIDTH[c])
        )
        post_rows(1, c)
        load_moment(c).start()
        if n == 0:
            post_flag(0)
        if n == 2:
            take(m1, mrecv_sem.at[1])
            post_names(2)
            take(flags.at[0], flag_sem.at[1, 0])
            flags[1, at[1]] = jnp.max(flags[0], axis=0)
        if n == 3:
            post_flag(1)
        if n == 5:
            take(flags.at[1], flag_sem.at[1, 1])
            flags[2, at[2]] = jnp.max(flags[1], axis=0)
        if n == 6:
            post_flag(2)
    wide.start()

    unit = lax.broadcasted_iota(jnp.int32, (64, 64), 0)
    slot_unit = (
        lax.broadcasted_iota(jnp.int32, (ROWS, 64), 0) // CAP == lax.broadcasted_iota(jnp.int32, (ROWS, 64), 1)
    ).astype(jnp.float32)
    slot = lax.broadcasted_iota(jnp.int32, (ROWS, 128), 0)
    for g, (a, b, c) in enumerate(ORDERS):
        take(ct2.at[g], ct_sem.at[3, g])
        c_unit = unit // 16
        a_unit, b_unit = ((unit // 4) % 4, unit % 4) if a < b else (unit % 4, (unit // 4) % 4)
        in_line = (coordinate(o_to, a) == at[a]) & (coordinate(o_to, b) == at[b])
        c_owner = coordinate(o_to, c)
        begin = jnp.zeros((64, 64), jnp.float32)
        size = jnp.zeros((64, 64), jnp.float32)
        for sb in range(4):
            for sa in range(4):
                row = jnp.broadcast_to(ct2[g, sb, sa].astype(jnp.float32), (64, 64))
                row = jnp.where(in_line & (b_unit == sb), row, 0.0)
                begin = begin + jnp.where(
                    (a_unit > sa) | ((a_unit == sa) & (c_owner < c_unit)), row, 0.0
                )
                size = size + jnp.where((a_unit == sa) & (c_owner == c_unit), row, 0.0)
        begin = jnp.dot(begin, ones, preferred_element_type=jnp.float32)
        size = jnp.dot(size, ones, preferred_element_type=jnp.float32)
        begin = jnp.dot(slot_unit, begin, preferred_element_type=jnp.float32)
        size = jnp.dot(slot_unit, size, preferred_element_type=jnp.float32)
        within = (slot % CAP).astype(jnp.float32)
        sb_slot = (slot // CAP) % 4 if a < b else (slot // (CAP * 4)) % 4
        comes = jnp.where(
            within < size, (sb_slot * LINE).astype(jnp.float32) + begin + within, -1.0
        )
        for q in range(0, 4 * LINE, 128):
            span = min(128, 4 * LINE - q)
            columns = (lax.broadcasted_iota(jnp.int32, (ROWS, span), 1) + q).astype(jnp.float32)
            unpack[g, :, pl.ds(q, span)] = (
                (columns == comes[:, :span]).astype(jnp.float32).astype(jnp.bfloat16)
            )

    for c in issue:
        take_rows(1, c)
        s2[c][...] = (
            jnp.dot(unpack[c // PER], r2[c][...].reshape(4 * LINE, WIDTH[c]), preferred_element_type=jnp.float32)
            .astype(jnp.bfloat16)
            .reshape(4, 4, 4, CAP, WIDTH[c])
        )
        post_rows(2, c)

    take(m1, mrecv_sem.at[2])
    named = m3[...].reshape(8, 8, 128).sum(axis=1)
    touched_parts = []
    for rb in range(8):
        rows = lax.broadcasted_iota(jnp.int32, (128, 128), 0) + (rb * 128 + 1)
        any_hit = jnp.zeros((128, 128), jnp.float32)
        for g in range(8):
            hit = (rows == named[g : g + 1, :]).astype(jnp.float32)
            onehot[pl.ds(rb * 128, 128), pl.ds(g * 128, 128)] = hit.astype(jnp.bfloat16)
            any_hit = jnp.maximum(any_hit, hit)
        hit_column = jnp.max(any_hit, axis=1, keepdims=True)
        touched_parts.append(hit_column)
        keep[pl.ds(rb * 128, 128), :] = jnp.broadcast_to(1.0 - 0.1 * hit_column, (128, 128))
    touched = to_row(jnp.concatenate(touched_parts, axis=0))
    steps = (rsteps[...] + 1).astype(jnp.float32)
    fix_first = 1.0 - jnp.exp(steps * jnp.log(jnp.float32(0.9)))
    fix_second = 1.0 - jnp.exp(steps * jnp.log(jnp.float32(0.95)))

    for n, c in enumerate(issue):
        take_rows(2, c)
        load_moment(c).wait()
        received = r3[c][...].reshape(ROWS, WIDTH[c])
        for rb in range(8):
            rows = pl.ds(rb * 128, 128)
            part = jnp.dot(onehot[rows, :], received, preferred_element_type=jnp.float32)
            folded = None
            for q in range(0, WIDTH[c], 128):
                columns = pl.ds(FIRST[c] + q, 128)
                piece = part[:, q : q + 128]
                first[rows, columns] = (
                    keep[rows, :] * tgv[c][rows, pl.ds(q, 128)].astype(jnp.float32) + 0.1 * piece
                )
                folded = piece * piece if folded is None else folded + piece * piece
            if n == 0:
                acc[rows, :] = folded
            else:
                acc[rows, :] += folded

    mine = to_row(jnp.sum(acc[...], axis=1, keepdims=True))
    sq_out[...] = mine
    swap = pltpu.make_async_remote_copy(
        src_ref=sq_out, dst_ref=sq_in, send_sem=sq_sem.at[0], recv_sem=sq_sem.at[1],
        device_id=partner, device_id_type=MESH,
    )
    swap.start()

    for phase in range(3):
        for c in range(CHUNKS):
            take(staged[phase][c], send_sem.at[phase, c])
        take(m1, msend_sem.at[phase])
        take(ct1.at[0], ct_sem.at[0, phase])
        take(ct2.at[0], ct_sem.at[2, phase])
        take(flags.at[0], flag_sem.at[0, phase])
    take(flags.at[2], flag_sem.at[1, 2])
    over[...] = jnp.max(flags[2], axis=0)
    wide.wait()
    swap.wait()

    square = (mine + sq_in[...]) / D
    live = touched > 0.0
    second = jnp.where(live, 0.95 * rscale[...] + 0.05 * square, rscale[...])
    scale[...] = second
    denom = jnp.sqrt(second / fix_second) + 1e-08
    rate = jnp.where(live, 0.01 / (fix_first * denom), 0.0)
    decay = jnp.where(live, 1.0 - 0.01 * 0.1, 1.0)
    eye = lax.broadcasted_iota(jnp.int32, (128, 128), 0) == lax.broadcasted_iota(jnp.int32, (128, 128), 1)
    for g in range(8):
        for i, value in enumerate((decay, rate)):
            column = jnp.sum(jnp.where(eye, value[g : g + 1, :], 0.0), axis=1, keepdims=True)
            coef[i, pl.ds(g * 128, 128), :] = jnp.broadcast_to(column, (128, 128))


def update(first, coef, scale, weights, new_weights, new_moment, new_scale, made_w, made_m, sem, scale_sem):
    out_scale = pltpu.make_async_copy(scale, new_scale, scale_sem)
    out_scale.start()
    copies = []
    for n in range(ROWS // TALL):
        block = pl.ds(n * TALL, TALL)

        def some(r, carry, n=n):
            rows = pl.ds(pl.multiple_of(n * TALL + r * 16, 16), 16)
            decay, rate = coef[0, rows, :], coef[1, rows, :]
            for q in range(0, HALF, 128):
                columns = pl.ds(q, 128)
                value = first[rows, columns]
                made_m[rows, columns] = value.astype(jnp.bfloat16)
                old = weights[rows, columns].astype(jnp.float32)
                made_w[rows, columns] = (decay * old - rate * value).astype(jnp.bfloat16)
            return carry

        lax.fori_loop(0, TALL // 16, some, 0)
        for i, (src, dst) in enumerate(((made_m, new_moment), (made_w, new_weights))):
            copy = pltpu.make_async_copy(src.at[block, :], dst.at[block, :], sem.at[i, n])
            copy.start()
            copies.append(copy)
    for copy in copies:
        copy.wait()
    out_scale.wait()


def over_pieces(value, axis):
    parts = lax.all_gather(value, axis)
    return parts.sum(axis=0)


def any_counts(token_grads, token_slot, slot_rows, counts, weights, moment, row_scale, row_steps):
    owners = lax.axis_size("vocab")
    slots_all = slot_rows.shape[1]
    cap = slots_all // owners
    half = token_grads.shape[1]
    rows_own = weights.shape[0]
    placing = token_slot[None, :] == jnp.arange(slots_all, dtype=jnp.int32)[:, None]
    slot_grads = jnp.dot(
        placing.astype(jnp.bfloat16), token_grads, preferred_element_type=jnp.float32
    ).astype(jnp.bfloat16)
    within = jnp.arange(cap, dtype=jnp.int32)
    live = within[None, :] < counts[0][:, None]
    named = jnp.where(live, slot_rows[0].reshape(owners, cap), -1)
    outgoing = slot_grads.reshape(owners, cap, half)
    received, received_rows = (
        lax.all_to_all(outgoing, "vocab", split_axis=0, concat_axis=0, tiled=True),
        lax.all_to_all(named, "vocab", split_axis=0, concat_axis=0, tiled=True),
    )
    flat = received.reshape(owners * cap, half)
    flat_rows = received_rows.reshape(owners * cap)
    table = flat_rows[None, :] == jnp.arange(rows_own, dtype=jnp.int32)[:, None]
    grad = jnp.dot(table.astype(jnp.bfloat16), flat, preferred_element_type=jnp.float32)
    hits = jnp.sum(table.astype(jnp.int32), axis=1)
    touched = hits > 0
    partial_sum = jnp.sum(grad * grad, axis=1)
    square = over_pieces(partial_sum, "width") / D
    step_count = (row_steps + 1).astype(jnp.float32)
    old_moment = moment.astype(jnp.float32)
    first = jnp.where(touched[:, None], 0.9 * old_moment + 0.1 * grad, old_moment)
    second = jnp.where(touched, 0.95 * row_scale + 0.05 * square, row_scale)
    fix_first = 1.0 - jnp.power(jnp.float32(0.9), step_count)
    fix_second = 1.0 - jnp.power(jnp.float32(0.95), step_count)
    denom = jnp.sqrt(second / fix_second) + 1e-08
    old = weights.astype(jnp.float32)
    stepped = old - 0.01 * (first / fix_first[:, None] / denom[:, None] + 0.1 * old)
    new_weights = jnp.where(touched[:, None], stepped, old).astype(jnp.bfloat16)
    return (new_weights, first.astype(jnp.bfloat16), second)


def shards(token_grads, token_slot, slot_rows, counts, weights, moment, row_scale, row_steps):
    vmem = pl.BlockSpec(memory_space=pltpu.VMEM)
    hbm = pl.BlockSpec(memory_space=pltpu.HBM)
    bf16, f32, i32 = jnp.bfloat16, jnp.float32, jnp.int32
    blocks = tuple(pltpu.VMEM((4, 4, 4, CAP, w), bf16) for w in WIDTH)
    first, coef, scale, weights_v, over = pl.pallas_call(
        exchange,
        name="exchange",
        out_shape=(
            pltpu.VMEM((ROWS, HALF), f32),
            pltpu.VMEM((2, ROWS, 128), f32),
            pltpu.VMEM((8, 128), f32),
            pltpu.VMEM((ROWS, HALF), bf16),
            jax.ShapeDtypeStruct((1, 128), i32),
        ),
        in_specs=[hbm] * 8,
        out_specs=(vmem,) * 5,
        scratch_shapes=[
            pltpu.VMEM((8, 128), i32),
            pltpu.VMEM((1, 1024), i32),
            pltpu.VMEM((1, 64), i32),
            pltpu.VMEM((8, 128), f32),
            pltpu.VMEM((8, 128), i32),
            pltpu.VMEM((ROWS, 128), f32),
            tuple(pltpu.VMEM((ROWS, w), bf16) for w in WIDTH),
            tuple(pltpu.VMEM((4, PLANE, w), bf16) for w in WIDTH),
            tuple(pltpu.VMEM((4, PLANE, w), bf16) for w in WIDTH),
            tuple(pltpu.VMEM((4, LINE, w), bf16) for w in WIDTH),
            tuple(pltpu.VMEM((4, LINE, w), bf16) for w in WIDTH),
            blocks,
            blocks,
            pltpu.VMEM((ROWS, ROWS), bf16),
            pltpu.VMEM((GROUPS, 4 * PLANE, ROWS), bf16),
            pltpu.VMEM((GROUPS, 4 * LINE, 4 * PLANE), bf16),
            pltpu.VMEM((GROUPS, ROWS, 4 * LINE), bf16),
            pltpu.VMEM((8, 8, 128), f32),
            pltpu.VMEM((3, 4, 1, 64), i32),
            pltpu.VMEM((3, 4, 4, 1, 64), i32),
            pltpu.VMEM((3, 4, 1, 128), i32),
            pltpu.VMEM((4, 4, 4, 1, 128), i32),
            pltpu.VMEM((4, 4, 4, 1, 128), i32),
            pltpu.VMEM((4, 4, 4, 1, 128), i32),
            pltpu.VMEM((4, 4, 4, 1, 128), i32),
            pltpu.VMEM((ROWS, 128), f32),
            pltpu.VMEM((8, 128), f32),
            pltpu.VMEM((8, 128), f32),
            pltpu.SemaphoreType.DMA((5,)),
            pltpu.SemaphoreType.DMA,
            pltpu.SemaphoreType.DMA((CHUNKS,)),
            pltpu.SemaphoreType.DMA((CHUNKS,)),
            pltpu.SemaphoreType.DMA((3, CHUNKS)),
            pltpu.SemaphoreType.DMA((3, CHUNKS)),
            pltpu.SemaphoreType.DMA((3,)),
            pltpu.SemaphoreType.DMA((3,)),
            pltpu.SemaphoreType.DMA((2,)),
            pltpu.SemaphoreType.DMA((4, 3)),
            pltpu.SemaphoreType.DMA((2, 3)),
        ],
        compiler_params=pltpu.CompilerParams(
            collective_id=0, has_side_effects=True, vmem_limit_bytes=46 * 1024 * 1024
        ),
        cost_estimate=pl.CostEstimate(flops=10**10, bytes_accessed=2 * 10**7, transcendentals=0),
    )(*(
        pltpu.with_memory_space_constraint(value, pltpu.HBM)
        for value in (
            token_grads, token_slot.reshape(8, 128), slot_rows, counts,
            row_scale.reshape(8, 128), row_steps.reshape(8, 128), weights, moment,
        )
    ))
    new_weights, new_moment, new_scale = pl.pallas_call(
        update,
        name="update",
        out_shape=(
            jax.ShapeDtypeStruct((ROWS, HALF), bf16),
            jax.ShapeDtypeStruct((ROWS, HALF), bf16),
            jax.ShapeDtypeStruct((8, 128), f32),
        ),
        in_specs=[vmem] * 4,
        out_specs=(hbm,) * 3,
        scratch_shapes=[
            pltpu.VMEM((ROWS, HALF), bf16),
            pltpu.VMEM((ROWS, HALF), bf16),
            pltpu.SemaphoreType.DMA((2, ROWS // TALL)),
            pltpu.SemaphoreType.DMA,
        ],
        compiler_params=pltpu.CompilerParams(vmem_limit_bytes=12 * 1024 * 1024),
        cost_estimate=pl.CostEstimate(flops=2 * 10**7, bytes_accessed=3 * 10**7, transcendentals=0),
    )(first, coef, scale, weights_v)
    arguments = (token_grads, token_slot, slot_rows, counts, weights, moment, row_scale, row_steps)
    return lax.while_loop(
        lambda state: state[3] > 0,
        lambda state: any_counts(*arguments) + (jnp.int32(0),),
        (new_weights, new_moment, new_scale.reshape(ROWS), over[0, 0]),
    )[:3]


def solution(mesh):
    return jax.shard_map(
        shards,
        mesh=mesh,
        in_specs=(
            P("vocab", "width"),
            P("vocab"),
            P("vocab", None),
            P("vocab", None),
            P("vocab", "width"),
            P("vocab", "width"),
            P("vocab"),
            P("vocab"),
        ),
        out_specs=(P("vocab", "width"), P("vocab", "width"), P("vocab")),
        check_vma=False,
    )
```
